256 devices in a mesh: gx: 16 (over y_hi, x, core), gy: 16 (over y_lo, z).
Axes of the slice: x: 4, y: 4 (y_hi: 2, y_lo: 2; y = y_hi * 2 + y_lo), z: 8, core: 2. Of those that a mesh axis runs over, the one named last changes fastest.
Arguments:
- right_side: float32 [3, 256, 128, 256], P(None, 'gx', 'gy'), may hold values from -12 to 12
- labels: int32 [256, 128, 256], P('gx', 'gy'), may hold values 0 or 1
Outputs:
- solution: float32 [3, 256, 128, 256], P(None, 'gx', 'gy')
- residual: float32 [3, 256, 128, 256], P(None, 'gx', 'gy')
The draws below stay inside these ranges and needn't reach their ends.
All inputs are finite; a program needn't handle non-finite values. No bound on the sum of `labels` on one device may be relied on, other than what follows from the above.
Results may differ from the reference program's by a relative error of at most 0.0003.
Values sent between devices are 32-bit elements; how exact they have to be, the bound alone decides.
A program may use at most 64 MiB of HBM per device.

```python
import math
import jax
import jax.numpy as jnp
import numpy as np
from jax import lax

NZ = 256
ITERS = 4
NX = 256
NY = 128


def draw_right_side(key, part):
    key_base = jax.random.fold_in(jax.random.fold_in(key, 11), 0)
    position_x = jnp.arange(NX, dtype=jnp.float32) / NX
    position_y = jnp.arange(NY, dtype=jnp.float32) / NY
    base_values = jnp.clip(jax.random.normal(key_base, (3, NX, NY, NZ), jnp.float32), -4.0, 4.0)
    amplitude = jnp.exp(math.log(3.0) * (0.5 * position_x[:, None] + 0.5 * position_y[None, :]))
    values = base_values * amplitude[None, :, :, None]
    return values.astype(jnp.float32)


def place_ends(entries, own_key, smallest, largest):
    dims = entries.shape
    spot = [jax.random.randint(jax.random.fold_in(own_key, axis), (), 0, dims[axis]) for axis in range(len(dims))]
    entries = entries.at[tuple(spot)].set(smallest)
    longest = dims.index(max(dims))
    spot[longest] = (spot[longest] + 1) % dims[longest]
    return entries.at[tuple(spot)].set(largest)


def setup_inputs(seed: int = 0) -> dict:
    key_list = jax.random.split(jax.random.key(seed), 3)
    return {
        "right_side": draw_right_side(jax.random.fold_in(key_list[2], 71), 0),
        "labels": place_ends((jax.random.randint(key_list[1], (NX, NY, NZ), 0, 3) < 1).astype(jnp.int32), jax.random.fold_in(key_list[1], 1), 0, 1),
    }


LAMBDA_SOFT = 0.5769231
LAMBDA_RISE = 1.6452991
SHEAR_SOFT = 0.3846154
SHEAR_RISE = 2.9487179
KAPPA = 0.05

def corner_bits(corner):
    return (corner >> 2 & 1, corner >> 1 & 1, corner & 1)

def element_tables():
    gauss_offset = 0.5 / math.sqrt(3.0)
    gauss_points = [0.5 - gauss_offset, 0.5 + gauss_offset]
    lame_table = np.zeros((24, 24))
    shear_table = np.zeros((24, 24))
    normal_block = np.zeros((6, 6))
    normal_block[:3, :3] = 1.0
    shear_block = np.zeros((6, 6))
    for entry in range(6):
        shear_block[entry, entry] = 2.0 if entry < 3 else 1.0
    for point_x in gauss_points:
        for point_y in gauss_points:
            for point_z in gauss_points:
                strain = np.zeros((6, 24))
                for corner in range(8):
                    cx_bit, cy_bit, cz_bit = corner_bits(corner)
                    shape_x = point_x if cx_bit else 1.0 - point_x
                    shape_y = point_y if cy_bit else 1.0 - point_y
                    shape_z = point_z if cz_bit else 1.0 - point_z
                    slope_x = 1.0 if cx_bit else -1.0
                    slope_y = 1.0 if cy_bit else -1.0
                    slope_z = 1.0 if cz_bit else -1.0
                    grad_x = slope_x * shape_y * shape_z
                    grad_y = shape_x * slope_y * shape_z
                    grad_z = shape_x * shape_y * slope_z
                    column = 3 * corner
                    strain[0, column] = grad_x
                    strain[1, column + 1] = grad_y
                    strain[2, column + 2] = grad_z
                    strain[3, column + 1] = grad_z
                    strain[3, column + 2] = grad_y
                    strain[4, column] = grad_z
                    strain[4, column + 2] = grad_x
                    strain[5, column] = grad_y
                    strain[5, column + 1] = grad_x
                lame_table += 0.125 * strain.T @ normal_block @ strain
                shear_table += 0.125 * strain.T @ shear_block @ strain
    return np.concatenate([lame_table, shear_table], 0).astype(np.float32)

def table_diagonal(table):
    return np.array([table[entry, entry] for entry in range(24)], dtype=np.float32)

def moduli(labels):
    stiff = labels.astype(jnp.float32)
    return (LAMBDA_SOFT + LAMBDA_RISE * stiff, SHEAR_SOFT + SHEAR_RISE * stiff)

def reference(right_side, labels):
    tables = element_tables()
    stiffness = jnp.asarray(tables, dtype=jnp.float32)
    diag_lame = jnp.asarray(table_diagonal(tables[:24]), dtype=jnp.float32)
    diag_shear = jnp.asarray(table_diagonal(tables[24:]), dtype=jnp.float32)
    lame_first, shear_modulus = moduli(labels)
    row_block = math.gcd(NX, 8)
    block_count = NX // row_block

    def operate(vector_in):
        wrapped = jnp.concatenate([vector_in, vector_in[:, :1]], 1)

        def one_block(number):
            offset = number * row_block
            node_values = lax.dynamic_slice_in_dim(wrapped, offset, row_block + 1, 1)
            lame_block = lax.dynamic_slice_in_dim(lame_first, offset, row_block, 0)
            shear_part = lax.dynamic_slice_in_dim(shear_modulus, offset, row_block, 0)
            rolled_z = jnp.roll(node_values, -1, 3)
            corner_views = []
            for corner in range(8):
                cx_bit, cy_bit, cz_bit = corner_bits(corner)
                source_nodes = rolled_z if cz_bit else node_values
                corner_view = source_nodes[:, cx_bit:cx_bit + row_block]
                if cy_bit:
                    corner_view = jnp.roll(corner_view, -1, 2)
                corner_views.append(corner_view)
            stacked = jnp.concatenate(corner_views, 0).reshape(24, -1)
            products = jnp.dot(stiffness, stacked, precision=lax.Precision.HIGHEST, preferred_element_type=jnp.float32)
            forces = (lame_block.reshape(1, -1) * products[:24] + shear_part.reshape(1, -1) * products[24:]).reshape(8, 3, row_block, NY, NZ)
            lower_sum = jnp.zeros((3, row_block, NY, NZ), jnp.float32)
            upper_sum = jnp.zeros((3, row_block, NY, NZ), jnp.float32)
            for corner in range(8):
                cx_bit, cy_bit, cz_bit = corner_bits(corner)
                portion = forces[corner]
                if cy_bit:
                    portion = jnp.roll(portion, 1, 2)
                if cz_bit:
                    portion = jnp.roll(portion, 1, 3)
                if cx_bit:
                    upper_sum = upper_sum + portion
                else:
                    lower_sum = lower_sum + portion
            return (lower_sum, upper_sum)
        lower_sum, upper_sum = lax.map(one_block, jnp.arange(block_count, dtype=jnp.int32))
        lower_sum = jnp.moveaxis(lower_sum, 0, 1).reshape(3, NX, NY, NZ)
        upper_sum = jnp.moveaxis(upper_sum, 0, 1).reshape(3, NX, NY, NZ)
        return lower_sum + jnp.roll(upper_sum, 1, 1) + KAPPA * vector_in
    diagonal = jnp.zeros((3, NX, NY, NZ), jnp.float32) + KAPPA
    for corner in range(8):
        cx_bit, cy_bit, cz_bit = corner_bits(corner)
        portion = lame_first[None] * diag_lame[3 * corner:3 * corner + 3, None, None, None] + shear_modulus[None] * diag_shear[3 * corner:3 * corner + 3, None, None, None]
        portion = jnp.roll(portion, (cx_bit, cy_bit, cz_bit), (1, 2, 3))
        diagonal = diagonal + portion
    solution = jnp.zeros_like(right_side)
    residual = right_side
    scaled = residual / diagonal
    direction = scaled
    descent = jnp.sum(residual * scaled)
    for iteration in range(ITERS):
        image_vector = operate(direction)
        step_length = descent / jnp.sum(direction * image_vector)
        solution = solution + step_length * direction
        residual = residual - step_length * image_vector
        scaled = residual / diagonal
        descent_new = jnp.sum(residual * scaled)
        direction = scaled + descent_new / descent * direction
        descent = descent_new
    return (solution, residual)
```

```python
import jax
import jax.numpy as jnp
from jax import lax
from jax.experimental import pallas as pl
from jax.experimental.pallas import tpu as pltpu
from jax.sharding import PartitionSpec as P

MESH = pl.DeviceIdType.MESH
ITERS = 4
LAMBDA_SOFT = 0.5769231
LAMBDA_RISE = 1.6452991
SHEAR_SOFT = 0.3846154
SHEAR_RISE = 2.9487179
KAPPA = 0.05

NX, NY, NZ = 16, 8, 256
HALO = 4
PX = NX + 2 * HALO
PY = 16
GROUP = 16
SIGMA = 1.05
RAW = 16.0
STEP = 2.0 / (RAW * SIGMA)

DIRECTIONS = [(1, 0), (1, 1), (1, -1), (0, 1), (0, -1), (-1, 0), (-1, 1), (-1, -1)]
DOTS = [(0, 0), (0, 1), (1, 1), (1, 2), (2, 2), (2, 3), (3, 3), (3, 4)]


def phases(form):
    soft = form(LAMBDA_SOFT, SHEAR_SOFT)
    stiff = form(LAMBDA_SOFT + LAMBDA_RISE, SHEAR_SOFT + SHEAR_RISE)
    return soft, stiff


def pick(stiff_mask, form):
    soft, stiff = phases(form)
    return jnp.where(stiff_mask, jnp.float32(stiff), jnp.float32(soft))


def plane_modes(w_ref, plane, modes):
    for c in range(3):
        u = w_ref[c, plane]
        uz = pltpu.roll(u, NZ - 1, 1)
        s, d = u + uz, uz - u
        sy, dy = pltpu.roll(s, PY - 1, 0), pltpu.roll(d, PY - 1, 0)
        modes[4 * c] = s + sy
        modes[4 * c + 1] = sy - s
        modes[4 * c + 2] = d + dy
        modes[4 * c + 3] = dy - d


def voxel_forces(plane, label_ref, lower, upper, carry, total):
    for row in (0, 8):
        for lane in (0, 128):
            at = (slice(row, row + 8), slice(lane, lane + 128))
            stiff = label_ref[plane, at[0], at[1]] > 0
            lam = pick(stiff, lambda la, mu: la)
            mu = pick(stiff, lambda la, mu: mu)
            mu2 = pick(stiff, lambda la, mu: 2.0 * mu)
            lam3 = pick(stiff, lambda la, mu: la / 3.0)
            mu3 = pick(stiff, lambda la, mu: mu / 3.0)
            dd9 = pick(stiff, lambda la, mu: (la + 4.0 * mu) / 9.0)
            a = [lower[i, at[0], at[1]] for i in range(12)]
            b = [upper[i, at[0], at[1]] for i in range(12)]
            d = [[b[4 * c + m] - a[4 * c + m] for m in range(4)] for c in range(3)]
            s = [[a[4 * c + m] + b[4 * c + m] if m else None for m in range(4)] for c in range(3)]
            fd = [[None] * 4 for _ in range(3)]
            fs = [[None] * 4 for _ in range(3)]
            trace = lam * (d[0][0] + s[1][1] + s[2][2])
            fd[0][0] = trace + mu2 * d[0][0]
            fs[1][1] = trace + mu2 * s[1][1]
            fs[2][2] = trace + mu2 * s[2][2]
            fd[1][0] = fs[0][1] = mu * (d[1][0] + s[0][1])
            fd[2][0] = fs[0][2] = mu * (d[2][0] + s[0][2])
            fs[2][1] = fs[1][2] = mu * (s[2][1] + s[1][2])
            h = lam3 * (d[0][1] + s[2][3])
            fd[0][1], fs[2][3] = h + mu * d[0][1], h + mu * s[2][3]
            h = lam3 * (d[0][2] + s[1][3])
            fd[0][2], fs[1][3] = h + mu * d[0][2], h + mu * s[1][3]
            h = lam3 * (d[1][1] + d[2][2])
            fd[1][1], fd[2][2] = h + mu * d[1][1], h + mu * d[2][2]
            three = s[0][3] + d[1][2] + d[2][1]
            fs[0][3] = mu3 * (s[0][3] + three)
            fd[1][2] = mu3 * (d[1][2] + three)
            fd[2][1] = mu3 * (d[2][1] + three)
            for c in range(3):
                fd[c][3] = dd9 * d[c][3]
            for c in range(3):
                for m in range(4):
                    i = 4 * c + m
                    before = carry[i, at[0], at[1]]
                    if m == 0:
                        total[i, at[0], at[1]] = before - fd[c][0]
                        carry[i, at[0], at[1]] = fd[c][0]
                    else:
                        total[i, at[0], at[1]] = before + (fs[c][m] - fd[c][m])
                        carry[i, at[0], at[1]] = fs[c][m] + fd[c][m]


def next_basis(plane, total, step_ref, shift_ref, w_ref, older_ref, out_ref):
    step, shift = step_ref[plane], shift_ref[plane]
    for c in range(3):
        mm, dm, md, dd = (total[4 * c + m] for m in range(4))
        p = (mm - dm) + pltpu.roll(mm + dm, 1, 0)
        q = (md - dd) + pltpu.roll(md + dd, 1, 0)
        force = (p - q) + pltpu.roll(p + q, 1, 1)
        value = step * force + shift * w_ref[c, plane]
        if older_ref is None:
            value = 0.5 * value
        else:
            value = value - older_ref[c, plane]
        out_ref[c, plane] = value


def coefficients(nu):
    half = 0.5

    def gram(i, j):
        return half * (nu[i + j] + nu[abs(i - j)])

    def image(p):
        out = [None] * (len(p) + 1)

        def add(i, value):
            out[i] = value if out[i] is None else out[i] + value

        for k, value in enumerate(p):
            whole, part = SIGMA * value, (0.5 * SIGMA) * value
            add(k, whole)
            if k == 0:
                add(1, whole)
            else:
                add(k + 1, part)
                add(k - 1, part)
        return out

    def form(u, v):
        total = None
        for i, ui in enumerate(u):
            row = None
            for j, vj in enumerate(v):
                term = gram(i, j) * vj
                row = term if row is None else row + term
            total = ui * row if total is None else total + ui * row
        return total

    one = jnp.ones_like(nu[0])
    solution, residual, direction = [], [one], [one]
    descent = gram(0, 0)
    for iteration in range(ITERS):
        moved = image(direction)
        step = descent / form(direction, moved)
        solution = [
            step * p + (solution[k] if k < len(solution) else 0.0) for k, p in enumerate(direction)
        ]
        residual = [
            (residual[k] - step * m) if k < len(residual) else -(step * m)
            for k, m in enumerate(moved)
        ]
        if iteration + 1 < ITERS:
            new = form(residual, residual)
            ratio = new / descent
            direction = [
                r + ratio * direction[k] if k < len(direction) else r
                for k, r in enumerate(residual)
            ]
            descent = new
    return solution, residual


def place(x, y, z, core):
    return {"gx": ((y // 2) * 4 + x) * 2 + core, "gy": lax.rem(y, 2) * 8 + z}


def kernel(r_hbm, l_hbm, sol_ref, res_ref, r_in, labels, diag, step_ref, shift_ref,
           w0, w1, w2, w3, w4, even, odd, carry, total,
           from_x, from_y, from_xy, mine, theirs,
           load_sem, send_sem, recv_sem, edge_send, edge_recv, sum_send, sum_recv):
    gx, gy = lax.axis_index("gx"), lax.axis_index("gy")
    core, x, y_hi = lax.rem(gx, 2), lax.rem(gx // 2, 4), gx // 8
    z, y_lo = lax.rem(gy, 8), gy // 8
    y = y_hi * 2 + y_lo

    own = (pl.ds(HALO, NX), pl.ds(0, NY))
    load_r = pltpu.make_async_copy(r_hbm, r_in.at[:, own[0], own[1]], load_sem.at[0])
    load_l = pltpu.make_async_copy(l_hbm, labels.at[own[0], own[1]], load_sem.at[1])
    load_r.start()
    load_l.start()

    def neighbour(dx, dy):
        return {"gx": lax.rem(gx + dx + GROUP, GROUP), "gy": lax.rem(gy + dy + GROUP, GROUP)}

    stages = [
        [place(lax.rem(x + k // 4, 4), lax.rem(y + k % 4, 4), z, core) for k in range(1, GROUP)],
        [place(x, y, lax.rem(z + k // 2, 8), lax.rem(core + k % 2, 2)) for k in range(1, GROUP)],
    ]
    barrier = pltpu.get_barrier_semaphore()
    greeted = [neighbour(dx, dy) for dx, dy in DIRECTIONS] + stages[0] + stages[1]
    for device in greeted:
        pl.semaphore_signal(barrier, inc=1, device_id=device, device_id_type=MESH)
    carry[...] = jnp.zeros_like(carry)
    load_r.wait()
    load_l.wait()
    pl.semaphore_wait(barrier, len(greeted))

    copies = []
    for number, (dx, dy) in enumerate(DIRECTIONS):
        xs = pl.ds({1: NX, 0: HALO, -1: HALO}[dx], NX if dx == 0 else HALO)
        xd = pl.ds({1: 0, 0: HALO, -1: HALO + NX}[dx], NX if dx == 0 else HALO)
        ys = pl.ds({1: 4, 0: 0, -1: 0}[dy], NY if dy == 0 else HALO)
        yd = pl.ds({1: 12, 0: 0, -1: 8}[dy], NY if dy == 0 else HALO)
        for kind, (source, target) in enumerate((
            (labels.at[xs, ys], labels.at[xd, yd]),
            (r_in.at[:, xs, ys], r_in.at[:, xd, yd]),
        )):
            copy = pltpu.make_async_remote_copy(
                src_ref=source, dst_ref=target,
                send_sem=send_sem.at[kind, number], recv_sem=recv_sem.at[kind, number],
                device_id=neighbour(dx, dy), device_id_type=MESH,
            )
            copy.start()
            copies.append(copy)
    for copy in copies:
        copy.wait()

    def corner_sums(plane):
        value = pick(labels[plane] > 0, lambda la, mu: (la + 4.0 * mu) / 9.0)
        value = value + pltpu.roll(value, 1, 1)
        return value + pltpu.roll(value, 1, 0)

    def diagonal_plane(plane, below):
        here = corner_sums(plane)
        value = here + below + KAPPA
        inverse = 1.0 / value
        diag[plane] = value
        step = STEP * inverse
        step_ref[plane] = step
        shift_ref[plane] = (RAW * KAPPA) * step - 2.0
        for c in range(3):
            w0[c, plane] = r_in[c, plane] * inverse
        return here

    lax.fori_loop(1, PX, diagonal_plane, corner_sums(0))

    def apply(first, last, w_ref, older_ref, out_ref):
        plane_modes(w_ref, first, even)

        def one(plane, lower, upper):
            plane_modes(w_ref, plane + 1, upper)
            voxel_forces(plane, labels, lower, upper, carry, total)
            next_basis(plane, total, step_ref, shift_ref, w_ref, older_ref, out_ref)

        def two(number, _):
            plane = first + 2 * number
            one(plane, even, odd)
            one(plane + 1, odd, even)
            return 0

        count = last - first + 1
        lax.fori_loop(0, count // 2, two, 0)
        if count % 2:
            one(last, even, odd)

    apply(1, 22, w0, None, w1)
    apply(2, 21, w1, w0, w2)
    apply(3, 20, w2, w1, w3)

    edges = [
        (w3.at[:, pl.ds(HALO + NX - 1, 1)], from_x, (1, 0)),
        (w3.at[:, pl.ds(HALO, NX + 1), pl.ds(NY - 1, 1)], from_y.at[:, :, pl.ds(NY - 1, 1)], (0, 1)),
        (w3.at[:, pl.ds(HALO + NX - 1, 1), pl.ds(0, NY)], from_xy, (1, 1)),
    ]
    copies = []
    for number, (source, target, (dx, dy)) in enumerate(edges):
        copy = pltpu.make_async_remote_copy(
            src_ref=source, dst_ref=target,
            send_sem=edge_send.at[number], recv_sem=edge_recv.at[number],
            device_id=neighbour(dx, dy), device_id_type=MESH,
        )
        copy.start()
        copies.append(copy)
    for copy in copies:
        copy.wait()
    for c in range(3):
        w3[c, HALO - 1, 0:8] = from_x[c, 0, 0:8]
        w3[c, HALO - 1, 8:16] = from_x[c, 0, 8:16]
        w3[c, HALO - 1, 15:16] = from_xy[c, 0, 7:8]
        for plane in range(NX + 1):
            w3[c, HALO + plane, 15:16] = from_y[c, plane, 7:8]
    apply(3, 19, w3, w2, w4)

    basis = (w0, w1, w2, w3, w4)

    def inner(number, sums):
        plane = HALO + number
        sums = list(sums)
        for c in range(3):
            for lane in (0, 128):
                at = (slice(0, NY), slice(lane, lane + 128))
                weight = diag[plane, at[0], at[1]]
                w = [ref[c, plane, at[0], at[1]] for ref in basis]
                scaled = [weight * v for v in w[:4]]
                for i, (j, k) in enumerate(DOTS):
                    sums[i] = sums[i] + scaled[j] * w[k]
        return tuple(sums)

    zero = jnp.zeros((NY, 128), jnp.float32)
    sums = lax.fori_loop(0, NX, inner, (zero,) * len(DOTS))
    lane = lax.broadcasted_iota(jnp.int32, (1, 128), 1)
    row = jnp.zeros((1, 128), jnp.float32)
    for i, value in enumerate(sums):
        value = jnp.sum(jnp.sum(value, axis=0, keepdims=True), axis=1, keepdims=True)
        row = jnp.where(lane == i, value, row)
    for stage, devices in enumerate(stages):
        mine[stage] = row
        copies = []
        for number, device in enumerate(devices):
            copy = pltpu.make_async_remote_copy(
                src_ref=mine.at[stage], dst_ref=theirs.at[stage, number],
                send_sem=sum_send.at[stage, number], recv_sem=sum_recv.at[stage, number],
                device_id=device, device_id_type=MESH,
            )
            copy.start()
            copies.append(copy)
        for copy in copies:
            copy.wait()
        for number in range(len(devices)):
            row = row + theirs[stage, number]
    dots = [
        jnp.sum(jnp.where(lane == i, row, 0.0), axis=1, keepdims=True) for i in range(len(DOTS))
    ]
    nu = [
        value if i < 2 else 2.0 * value - dots[i % 2] for i, value in enumerate(dots)
    ]
    solution, residual = coefficients(nu)
    solution = [jnp.broadcast_to(v, (NY, 128)) for v in solution]
    residual = [jnp.broadcast_to(v, (NY, 128)) for v in residual]

    def combine(number, _):
        plane = HALO + number
        for c in range(3):
            for lane in (0, 128):
                at = (slice(0, NY), slice(lane, lane + 128))
                w = [ref[c, plane, at[0], at[1]] for ref in basis]
                x = solution[0] * w[0]
                r = residual[0] * w[0]
                for k in range(1, 5):
                    if k < 4:
                        x = x + solution[k] * w[k]
                    r = r + residual[k] * w[k]
                sol_ref[c, number, at[0], at[1]] = x
                res_ref[c, number, at[0], at[1]] = diag[plane, at[0], at[1]] * r
        return 0

    lax.fori_loop(0, NX, combine, 0)


def local(right_side, labels):
    shape = (3, NX, NY, NZ)
    vector = pltpu.VMEM((3, PX, PY, NZ), jnp.float32)
    scalar = pltpu.VMEM((PX, PY, NZ), jnp.float32)
    modes = pltpu.VMEM((12, PY, NZ), jnp.float32)
    return pl.pallas_call(
        kernel,
        out_shape=(jax.ShapeDtypeStruct(shape, jnp.float32),) * 2,
        in_specs=[pl.BlockSpec(memory_space=pl.ANY)] * 2,
        out_specs=[pl.BlockSpec(memory_space=pltpu.VMEM)] * 2,
        scratch_shapes=[
            vector, pltpu.VMEM((PX, PY, NZ), jnp.int32), scalar, scalar, scalar,
            vector, vector, vector, vector, vector, modes, modes, modes, modes,
            pltpu.VMEM((3, 1, PY, NZ), jnp.float32),
            pltpu.VMEM((3, NX + 1, NY, NZ), jnp.float32),
            pltpu.VMEM((3, 1, NY, NZ), jnp.float32),
            pltpu.VMEM((2, 1, 128), jnp.float32),
            pltpu.VMEM((2, GROUP - 1, 1, 128), jnp.float32),
            pltpu.SemaphoreType.DMA((2,)),
            pltpu.SemaphoreType.DMA((2, 8)),
            pltpu.SemaphoreType.DMA((2, 8)),
            pltpu.SemaphoreType.DMA((3,)),
            pltpu.SemaphoreType.DMA((3,)),
            pltpu.SemaphoreType.DMA((2, GROUP - 1)),
            pltpu.SemaphoreType.DMA((2, GROUP - 1)),
        ],
        compiler_params=pltpu.CompilerParams(
            collective_id=0, has_side_effects=True, vmem_limit_bytes=40 * 1024 * 1024
        ),
    )(right_side, labels)


def solution(mesh):
    specs = P(None, "gx", "gy", None)
    return jax.shard_map(
        local, mesh=mesh, in_specs=(specs, P("gx", "gy", None)), out_specs=(specs, specs),
        check_vma=False,
    )
```

```python
import jax
import jax.numpy as jnp
from jax import lax
from jax.experimental import pallas as pl
from jax.experimental.pallas import tpu as pltpu
from jax.sharding import PartitionSpec as P

MESH = pl.DeviceIdType.MESH
ITERS = 4
LAMBDA_SOFT = 0.5769231
LAMBDA_RISE = 1.6452991
SHEAR_SOFT = 0.3846154
SHEAR_RISE = 2.9487179
KAPPA = 0.05

NX, NY, NZ = 16, 8, 256
HALO = 4
PX = NX + 2 * HALO
PY = 16
GROUP = 16
SIGMA = 1.05
RAW = 16.0
STEP = 2.0 / (RAW * SIGMA)

DIRECTIONS = [(1, 0), (1, 1), (1, -1), (-1, 0), (-1, 1), (-1, -1), (0, 1), (0, -1)]
DOTS = [(0, 0), (0, 1), (1, 1), (1, 2), (2, 2), (2, 3), (3, 3)]


def phases(form):
    soft = form(LAMBDA_SOFT, SHEAR_SOFT)
    stiff = form(LAMBDA_SOFT + LAMBDA_RISE, SHEAR_SOFT + SHEAR_RISE)
    return soft, stiff


def pick(stiff_mask, form):
    soft, stiff = phases(form)
    return jnp.where(stiff_mask, jnp.float32(stiff), jnp.float32(soft))


def plane_modes(w_ref, plane, modes):
    for c in range(3):
        u = w_ref[c, plane]
        uz = pltpu.roll(u, NZ - 1, 1)
        s, d = u + uz, uz - u
        sy, dy = pltpu.roll(s, PY - 1, 0), pltpu.roll(d, PY - 1, 0)
        modes[4 * c] = s + sy
        modes[4 * c + 1] = sy - s
        modes[4 * c + 2] = d + dy
        modes[4 * c + 3] = dy - d


def voxel_forces(plane, label_ref, lower, upper, carry, total):
    for row in (0, 8):
        for lane in (0, 128):
            at = (slice(row, row + 8), slice(lane, lane + 128))
            stiff = label_ref[plane, at[0], at[1]] > 0
            lam = pick(stiff, lambda la, mu: la)
            mu = pick(stiff, lambda la, mu: mu)
            mu2 = pick(stiff, lambda la, mu: 2.0 * mu)
            lam3 = pick(stiff, lambda la, mu: la / 3.0)
            mu3 = pick(stiff, lambda la, mu: mu / 3.0)
            dd9 = pick(stiff, lambda la, mu: (la + 4.0 * mu) / 9.0)
            a = [lower[i, at[0], at[1]] for i in range(12)]
            b = [upper[i, at[0], at[1]] for i in range(12)]
            d = [[b[4 * c + m] - a[4 * c + m] for m in range(4)] for c in range(3)]
            s = [[a[4 * c + m] + b[4 * c + m] if m else None for m in range(4)] for c in range(3)]
            fd = [[None] * 4 for _ in range(3)]
            fs = [[None] * 4 for _ in range(3)]
            trace = lam * (d[0][0] + s[1][1] + s[2][2])
            fd[0][0] = trace + mu2 * d[0][0]
            fs[1][1] = trace + mu2 * s[1][1]
            fs[2][2] = trace + mu2 * s[2][2]
            fd[1][0] = fs[0][1] = mu * (d[1][0] + s[0][1])
            fd[2][0] = fs[0][2] = mu * (d[2][0] + s[0][2])
            fs[2][1] = fs[1][2] = mu * (s[2][1] + s[1][2])
            h = lam3 * (d[0][1] + s[2][3])
            fd[0][1], fs[2][3] = h + mu * d[0][1], h + mu * s[2][3]
            h = lam3 * (d[0][2] + s[1][3])
            fd[0][2], fs[1][3] = h + mu * d[0][2], h + mu * s[1][3]
            h = lam3 * (d[1][1] + d[2][2])
            fd[1][1], fd[2][2] = h + mu * d[1][1], h + mu * d[2][2]
            three = s[0][3] + d[1][2] + d[2][1]
            fs[0][3] = mu3 * (s[0][3] + three)
            fd[1][2] = mu3 * (d[1][2] + three)
            fd[2][1] = mu3 * (d[2][1] + three)
            for c in range(3):
                fd[c][3] = dd9 * d[c][3]
            for c in range(3):
                for m in range(4):
                    i = 4 * c + m
                    before = carry[i, at[0], at[1]]
                    if m == 0:
                        total[i, at[0], at[1]] = before - fd[c][0]
                        carry[i, at[0], at[1]] = fd[c][0]
                    else:
                        total[i, at[0], at[1]] = before + (fs[c][m] - fd[c][m])
                        carry[i, at[0], at[1]] = fs[c][m] + fd[c][m]


def voxel_energy(plane, label_ref, at, lower, upper):
    stiff = label_ref[plane, at[0], at[1]] > 0
    lam = pick(stiff, lambda la, mu: la)
    mu = pick(stiff, lambda la, mu: mu)
    a = [lower[i, at[0], at[1]] for i in range(12)]
    b = [upper[i, at[0], at[1]] for i in range(12)]
    d = [[b[4 * c + m] - a[4 * c + m] for m in range(4)] for c in range(3)]
    s = [[a[4 * c + m] + b[4 * c + m] if m else None for m in range(4)] for c in range(3)]

    def squares(*values):
        total = None
        for v in values:
            total = v * v if total is None else total + v * v
        return total

    third, ninth = 1.0 / 3.0, 1.0 / 9.0
    corners = squares(d[0][3], d[1][3], d[2][3])
    pairs = ((d[0][1], s[2][3]), (d[0][2], s[1][3]), (d[1][1], d[2][2]))
    singles = (s[0][3], d[1][2], d[2][1])
    lam_part = (
        squares(d[0][0] + s[1][1] + s[2][2])
        + third * squares(*(p + q for p, q in pairs))
        + ninth * corners
    )
    mu_part = (
        2.0 * squares(d[0][0], s[1][1], s[2][2])
        + squares(d[1][0] + s[0][1], d[2][0] + s[0][2], s[2][1] + s[1][2])
        + squares(*(v for pair in pairs for v in pair))
        + third * (squares(*singles) + squares(singles[0] + singles[1] + singles[2]))
        + (4.0 * ninth) * corners
    )
    return lam * lam_part + mu * mu_part


def next_basis(plane, total, step_ref, shift_ref, w_ref, older_ref, out_ref):
    step, shift = step_ref[plane], shift_ref[plane]
    for c in range(3):
        mm, dm, md, dd = (total[4 * c + m] for m in range(4))
        p = (mm - dm) + pltpu.roll(mm + dm, 1, 0)
        q = (md - dd) + pltpu.roll(md + dd, 1, 0)
        force = (p - q) + pltpu.roll(p + q, 1, 1)
        value = step * force + shift * w_ref[c, plane]
        if older_ref is None:
            value = 0.5 * value
        else:
            value = value - older_ref[c, plane]
        out_ref[c, plane] = value


def coefficients(nu):
    half = 0.5

    def gram(i, j):
        return half * (nu[i + j] + nu[abs(i - j)])

    def image(p):
        out = [None] * (len(p) + 1)

        def add(i, value):
            out[i] = value if out[i] is None else out[i] + value

        for k, value in enumerate(p):
            whole, part = SIGMA * value, (0.5 * SIGMA) * value
            add(k, whole)
            if k == 0:
                add(1, whole)
            else:
                add(k + 1, part)
                add(k - 1, part)
        return out

    def form(u, v):
        total = None
        for i, ui in enumerate(u):
            row = None
            for j, vj in enumerate(v):
                term = gram(i, j) * vj
                row = term if row is None else row + term
            total = ui * row if total is None else total + ui * row
        return total

    one = jnp.ones_like(nu[0])
    solution, residual, direction = [], [one], [one]
    descent = gram(0, 0)
    for iteration in range(ITERS):
        moved = image(direction)
        step = descent / form(direction, moved)
        solution = [
            step * p + (solution[k] if k < len(solution) else 0.0) for k, p in enumerate(direction)
        ]
        residual = [
            (residual[k] - step * m) if k < len(residual) else -(step * m)
            for k, m in enumerate(moved)
        ]
        if iteration + 1 < ITERS:
            new = form(residual, residual)
            ratio = new / descent
            direction = [
                r + ratio * direction[k] if k < len(direction) else r
                for k, r in enumerate(residual)
            ]
            descent = new
    return solution, residual


def place(x, y, z, core):
    return {"gx": ((y // 2) * 4 + x) * 2 + core, "gy": lax.rem(y, 2) * 8 + z}


def kernel(r_hbm, l_hbm, sol_ref, res_ref, r_in, labels, diag, step_ref, shift_ref, below,
           w0, w1, w2, w3, w4, *rest):
    sets, rest = [rest[4 * k : 4 * k + 4] for k in range(3)], rest[12:]
    (from_x, from_y, from_xy, mine, theirs, load_sem, send_sem, recv_sem,
     face_send, face_recv, edge_send, edge_recv, sum_send, sum_recv) = rest
    gx, gy = lax.axis_index("gx"), lax.axis_index("gy")
    core, x, y_hi = lax.rem(gx, 2), lax.rem(gx // 2, 4), gx // 8
    z, y_lo = lax.rem(gy, 8), gy // 8
    y = y_hi * 2 + y_lo

    def neighbour(dx, dy):
        return {"gx": lax.rem(gx + dx + GROUP, GROUP), "gy": lax.rem(gy + dy + GROUP, GROUP)}

    stages = [
        [place(lax.rem(x + k // 4, 4), lax.rem(y + k % 4, 4), z, core) for k in range(1, GROUP)],
        [place(x, y, lax.rem(z + k // 2, 8), lax.rem(core + k % 2, 2)) for k in range(1, GROUP)],
    ]
    barrier = pltpu.get_barrier_semaphore()
    greeted = [neighbour(dx, dy) for dx, dy in DIRECTIONS] + stages[0] + stages[1]
    for device in greeted:
        pl.semaphore_signal(barrier, inc=1, device_id=device, device_id_type=MESH)
    own = (pl.ds(HALO, NX), pl.ds(0, NY))
    load_r = pltpu.make_async_copy(r_hbm, r_in.at[:, own[0], own[1]], load_sem.at[0])
    load_l = pltpu.make_async_copy(l_hbm, labels.at[own[0], own[1]], load_sem.at[1])
    load_r.start()
    load_l.start()
    load_r.wait()
    load_l.wait()
    pl.semaphore_wait(barrier, len(greeted))

    def piece(xs, ys, xd, yd, device, sends, recvs):
        pairs = ((labels.at[xs, ys], labels.at[xd, yd]), (r_in.at[:, xs, ys], r_in.at[:, xd, yd]))
        return [
            pltpu.make_async_remote_copy(
                src_ref=source, dst_ref=target, send_sem=sends(kind), recv_sem=recvs(kind),
                device_id=device, device_id_type=MESH,
            )
            for kind, (source, target) in enumerate(pairs)
        ]

    def rows(dy):
        return (pl.ds({1: 4, 0: 0, -1: 0}[dy], NY if dy == 0 else 4),
                pl.ds({1: 12, 0: 0, -1: 8}[dy], NY if dy == 0 else 4))

    def slab(number):
        dx, dy = DIRECTIONS[number]
        ys, yd = rows(dy)
        return piece(
            pl.ds(NX if dx == 1 else HALO, HALO), ys, pl.ds(0 if dx == 1 else HALO + NX, HALO), yd,
            neighbour(dx, dy),
            lambda kind: send_sem.at[kind, number], lambda kind: recv_sem.at[kind, number],
        )

    def face(part, side):
        ys, yd = rows(1 - 2 * side)
        at = pl.ds(HALO * part, HALO)
        return piece(
            at, ys, at, yd, neighbour(0, 1 - 2 * side),
            lambda kind: face_send.at[kind, side, part - 1],
            lambda kind: face_recv.at[kind, side, part - 1],
        )

    halo = []
    for number in (0, 1, 2):
        halo += slab(number)
    for part in range(1, 5):
        halo += face(part, 0) + face(part, 1)
    for number in (3, 4, 5):
        halo += slab(number)
    for copy in halo:
        copy.start()

    def corner_sums(plane):
        value = pick(labels[plane] > 0, lambda la, mu: (la + 4.0 * mu) / 9.0)
        value = value + pltpu.roll(value, 1, 1)
        return value + pltpu.roll(value, 1, 0)

    def diagonal_plane(plane):
        here = corner_sums(plane)
        value = here + below[...] + KAPPA
        below[...] = here
        inverse = 1.0 / value
        diag[plane] = value
        step = STEP * inverse
        step_ref[plane] = step
        shift_ref[plane] = (RAW * KAPPA) * step - 2.0
        for c in range(3):
            w0[c, plane] = r_in[c, plane] * inverse

    basis = (w0, w1, w2, w3, w4)

    def level(k, plane, parity):
        even, odd, carry, total = sets[k - 1]
        lower, upper = (even, odd) if parity == 0 else (odd, even)
        older = basis[k - 2] if k > 1 else None
        plane_modes(basis[k - 1], plane + 1, upper)
        voxel_forces(plane, labels, lower, upper, carry, total)
        next_basis(plane, total, step_ref, shift_ref, basis[k - 1], older, basis[k])

    for number in (0, 1, 2):
        for copy in slab(number):
            copy.wait_recv()
    below[...] = corner_sums(0)
    for p in range(1, 6):
        if p == 4:
            for side in (0, 1):
                for copy in face(1, side):
                    copy.wait_recv()
        diagonal_plane(p)
        for k in (1, 2, 3):
            if p == 2 * k - 1:
                plane_modes(basis[k - 1], k, sets[k - 1][k % 2])
            elif p >= 2 * k:
                level(k, p - k, (p - k) % 2)

    def two_planes(number, _):
        first = 6 + 2 * number

        @pl.when(lax.rem(first, 4) == 0)
        def _():
            @pl.when(first < HALO + NX)
            def _():
                for side in (0, 1):
                    for copy in face(first // 4, side):
                        copy.wait_recv()

            @pl.when(first == HALO + NX)
            def _():
                for number in (3, 4, 5):
                    for copy in slab(number):
                        copy.wait_recv()

        for extra in (0, 1):
            diagonal_plane(first + extra)
            for k in (1, 2, 3):
                level(k, first + extra - k, (extra - k) % 2)
        return 0

    lax.fori_loop(0, 9, two_planes, 0)

    edges = [
        (w3.at[:, pl.ds(HALO + NX - 1, 1)], from_x, (1, 0)),
        (w3.at[:, pl.ds(HALO, NX + 1), pl.ds(NY - 1, 1)], from_y.at[:, :, pl.ds(NY - 1, 1)], (0, 1)),
        (w3.at[:, pl.ds(HALO + NX - 1, 1), pl.ds(0, NY)], from_xy, (1, 1)),
    ]
    edge_copies = []
    for number, (source, target, (dx, dy)) in enumerate(edges):
        copy = pltpu.make_async_remote_copy(
            src_ref=source, dst_ref=target,
            send_sem=edge_send.at[number], recv_sem=edge_recv.at[number],
            device_id=neighbour(dx, dy), device_id_type=MESH,
        )
        copy.start()
        edge_copies.append(copy)

    zero = jnp.zeros((NY, 128), jnp.float32)
    even, odd, carry, total = sets[0]
    plane_modes(w3, HALO, even)

    def inner(plane, lower, upper, sums):
        sums = list(sums)
        plane_modes(w3, plane + 1, upper)
        for lane in (0, 128):
            at = (slice(0, NY), slice(lane, lane + 128))
            weight = diag[plane, at[0], at[1]]
            for c in range(3):
                w = [ref[c, plane, at[0], at[1]] for ref in basis[:4]]
                scaled = [weight * v for v in w]
                for i, (j, k) in enumerate(DOTS):
                    sums[i] = sums[i] + scaled[j] * w[k]
                sums[7] = sums[7] + (RAW * KAPPA) * (w[3] * w[3])
            sums[7] = sums[7] + voxel_energy(plane, labels, at, lower, upper)
        return tuple(sums)

    def inner_two(number, sums):
        plane = HALO + 2 * number
        sums = inner(plane, even, odd, sums)
        return inner(plane + 1, odd, even, sums)

    sums = lax.fori_loop(0, NX // 2, inner_two, (zero,) * 8)
    lane = lax.broadcasted_iota(jnp.int32, (1, 128), 1)
    row = jnp.zeros((1, 128), jnp.float32)
    for i, value in enumerate(sums):
        value = jnp.sum(jnp.sum(value, axis=0, keepdims=True), axis=1, keepdims=True)
        row = jnp.where(lane == i, value, row)

    def share(stage, row):
        mine[stage] = row
        copies = []
        for number, device in enumerate(stages[stage]):
            copy = pltpu.make_async_remote_copy(
                src_ref=mine.at[stage], dst_ref=theirs.at[stage, number],
                send_sem=sum_send.at[stage, number], recv_sem=sum_recv.at[stage, number],
                device_id=device, device_id_type=MESH,
            )
            copy.start()
            copies.append(copy)
        return copies

    def collect(stage, row, copies):
        for copy in copies:
            copy.wait()
        for number in range(len(copies)):
            row = row + theirs[stage, number]
        return row

    copies = share(0, row)
    for copy in halo:
        copy.wait_send()
    for copy in edge_copies:
        copy.wait()
    for c in range(3):
        w3[c, HALO - 1, 0:8] = from_x[c, 0, 0:8]
        w3[c, HALO - 1, 8:16] = from_x[c, 0, 8:16]
        w3[c, HALO - 1, 15:16] = from_xy[c, 0, 7:8]
        for plane in range(NX + 1):
            w3[c, HALO + plane, 15:16] = from_y[c, plane, 7:8]
    row = collect(0, row, copies)
    copies = share(1, row)

    def last_level(plane, lower, upper):
        plane_modes(w3, plane + 1, upper)
        voxel_forces(plane, labels, lower, upper, carry, total)
        next_basis(plane, total, step_ref, shift_ref, w3, w2, w4)

    def last_two(number, _):
        plane = HALO - 1 + 2 * number
        last_level(plane, even, odd)
        last_level(plane + 1, odd, even)
        return 0

    plane_modes(w3, HALO - 1, even)
    lax.fori_loop(0, NX // 2, last_two, 0)
    last_level(HALO + NX - 1, even, odd)

    row = collect(1, row, copies)
    dots = [
        jnp.sum(jnp.where(lane == i, row, 0.0), axis=1, keepdims=True) for i in range(8)
    ]
    last = (2.0 / (RAW * SIGMA)) * dots[7] - 2.0 * dots[6] - dots[5]
    nu = [
        dots[0], dots[1], 2.0 * dots[2] - dots[0], 2.0 * dots[3] - dots[1],
        2.0 * dots[4] - dots[0], 2.0 * dots[5] - dots[1], 2.0 * dots[6] - dots[0],
        2.0 * last - dots[1],
    ]
    solution, residual = coefficients(nu)
    solution = [jnp.broadcast_to(v, (NY, 128)) for v in solution]
    residual = [jnp.broadcast_to(v, (NY, 128)) for v in residual]

    def combine(number, _):
        plane = HALO + number
        for c in range(3):
            for lane in (0, 128):
                at = (slice(0, NY), slice(lane, lane + 128))
                w = [ref[c, plane, at[0], at[1]] for ref in basis]
                x = solution[0] * w[0]
                r = residual[0] * w[0]
                for k in range(1, 5):
                    if k < 4:
                        x = x + solution[k] * w[k]
                    r = r + residual[k] * w[k]
                sol_ref[c, number, at[0], at[1]] = x
                res_ref[c, number, at[0], at[1]] = diag[plane, at[0], at[1]] * r
        return 0

    lax.fori_loop(0, NX, combine, 0)


def local(right_side, labels):
    shape = (3, NX, NY, NZ)
    vector = pltpu.VMEM((3, PX, PY, NZ), jnp.float32)
    scalar = pltpu.VMEM((PX, PY, NZ), jnp.float32)
    modes = pltpu.VMEM((12, PY, NZ), jnp.float32)
    return pl.pallas_call(
        kernel,
        out_shape=(jax.ShapeDtypeStruct(shape, jnp.float32),) * 2,
        in_specs=[pl.BlockSpec(memory_space=pltpu.HBM)] * 2,
        out_specs=[pl.BlockSpec(memory_space=pltpu.VMEM)] * 2,
        scratch_shapes=[
            vector, pltpu.VMEM((PX, PY, NZ), jnp.int32), scalar, scalar, scalar,
            pltpu.VMEM((PY, NZ), jnp.float32),
            vector, vector, vector, vector, vector, *([modes] * 12),
            pltpu.VMEM((3, 1, PY, NZ), jnp.float32),
            pltpu.VMEM((3, NX + 1, NY, NZ), jnp.float32),
            pltpu.VMEM((3, 1, NY, NZ), jnp.float32),
            pltpu.VMEM((2, 1, 128), jnp.float32),
            pltpu.VMEM((2, GROUP - 1, 1, 128), jnp.float32),
            pltpu.SemaphoreType.DMA((2,)),
            pltpu.SemaphoreType.DMA((2, 6)),
            pltpu.SemaphoreType.DMA((2, 6)),
            pltpu.SemaphoreType.DMA((2, 2, 4)),
            pltpu.SemaphoreType.DMA((2, 2, 4)),
            pltpu.SemaphoreType.DMA((3,)),
            pltpu.SemaphoreType.DMA((3,)),
            pltpu.SemaphoreType.DMA((2, GROUP - 1)),
            pltpu.SemaphoreType.DMA((2, GROUP - 1)),
        ],
        compiler_params=pltpu.CompilerParams(
            collective_id=0, has_side_effects=True, vmem_limit_bytes=40 * 1024 * 1024
        ),
    )(right_side, labels)


def solution(mesh):
    specs = P(None, "gx", "gy", None)
    return jax.shard_map(
        local, mesh=mesh, in_specs=(specs, P("gx", "gy", None)), out_specs=(specs, specs),
        check_vma=False,
    )
```

```python
import jax
import jax.numpy as jnp
from jax import lax
from jax.experimental import pallas as pl
from jax.experimental.pallas import tpu as pltpu
from jax.sharding import PartitionSpec as P

MESH = pl.DeviceIdType.MESH
ITERS = 4
LAMBDA_SOFT = 0.5769231
LAMBDA_RISE = 1.6452991
SHEAR_SOFT = 0.3846154
SHEAR_RISE = 2.9487179
KAPPA = 0.05

NX, NY, NZ = 16, 8, 256
HALO = 4
PX = NX + 2 * HALO
PY = 16
GROUP = 16
SIGMA = 1.05
RAW = 16.0
STEP = 2.0 / (RAW * SIGMA)

DIRECTIONS = [(1, 0), (1, 1), (1, -1), (-1, 0), (-1, 1), (-1, -1), (0, 1), (0, -1)]
DOTS = [(0, 0), (0, 1), (1, 1), (1, 2), (2, 2), (2, 3), (3, 3)]


def phases(form):
    soft = form(LAMBDA_SOFT, SHEAR_SOFT)
    stiff = form(LAMBDA_SOFT + LAMBDA_RISE, SHEAR_SOFT + SHEAR_RISE)
    return soft, stiff


def pick(stiff_mask, form):
    soft, stiff = phases(form)
    return jnp.where(stiff_mask, jnp.float32(stiff), jnp.float32(soft))


def plane_modes(w_ref, plane, modes):
    for c in range(3):
        u = w_ref[c, plane]
        uz = pltpu.roll(u, NZ - 1, 1)
        s, d = u + uz, uz - u
        sy, dy = pltpu.roll(s, PY - 1, 0), pltpu.roll(d, PY - 1, 0)
        modes[4 * c] = s + sy
        modes[4 * c + 1] = sy - s
        modes[4 * c + 2] = d + dy
        modes[4 * c + 3] = dy - d


def voxel_forces(plane, label_ref, lower, upper, carry, total):
    for row in (0, 8):
        for lane in (0, 128):
            at = (slice(row, row + 8), slice(lane, lane + 128))
            stiff = label_ref[plane, at[0], at[1]] > 0
            lam = pick(stiff, lambda la, mu: la)
            mu = pick(stiff, lambda la, mu: mu)
            mu2 = pick(stiff, lambda la, mu: 2.0 * mu)
            lam3 = pick(stiff, lambda la, mu: la / 3.0)
            mu3 = pick(stiff, lambda la, mu: mu / 3.0)
            dd9 = pick(stiff, lambda la, mu: (la + 4.0 * mu) / 9.0)
            a = [lower[i, at[0], at[1]] for i in range(12)]
            b = [upper[i, at[0], at[1]] for i in range(12)]
            d = [[b[4 * c + m] - a[4 * c + m] for m in range(4)] for c in range(3)]
            s = [[a[4 * c + m] + b[4 * c + m] if m else None for m in range(4)] for c in range(3)]
            fd = [[None] * 4 for _ in range(3)]
            fs = [[None] * 4 for _ in range(3)]
            trace = lam * (d[0][0] + s[1][1] + s[2][2])
            fd[0][0] = trace + mu2 * d[0][0]
            fs[1][1] = trace + mu2 * s[1][1]
            fs[2][2] = trace + mu2 * s[2][2]
            fd[1][0] = fs[0][1] = mu * (d[1][0] + s[0][1])
            fd[2][0] = fs[0][2] = mu * (d[2][0] + s[0][2])
            fs[2][1] = fs[1][2] = mu * (s[2][1] + s[1][2])
            h = lam3 * (d[0][1] + s[2][3])
            fd[0][1], fs[2][3] = h + mu * d[0][1], h + mu * s[2][3]
            h = lam3 * (d[0][2] + s[1][3])
            fd[0][2], fs[1][3] = h + mu * d[0][2], h + mu * s[1][3]
            h = lam3 * (d[1][1] + d[2][2])
            fd[1][1], fd[2][2] = h + mu * d[1][1], h + mu * d[2][2]
            three = s[0][3] + d[1][2] + d[2][1]
            fs[0][3] = mu3 * (s[0][3] + three)
            fd[1][2] = mu3 * (d[1][2] + three)
            fd[2][1] = mu3 * (d[2][1] + three)
            for c in range(3):
                fd[c][3] = dd9 * d[c][3]
            for c in range(3):
                for m in range(4):
                    i = 4 * c + m
                    before = carry[i, at[0], at[1]]
                    if m == 0:
                        total[i, at[0], at[1]] = before - fd[c][0]
                        carry[i, at[0], at[1]] = fd[c][0]
                    else:
                        total[i, at[0], at[1]] = before + (fs[c][m] - fd[c][m])
                        carry[i, at[0], at[1]] = fs[c][m] + fd[c][m]


def voxel_energy(plane, label_ref, at, lower, upper):
    stiff = label_ref[plane, at[0], at[1]] > 0
    lam = pick(stiff, lambda la, mu: la)
    mu = pick(stiff, lambda la, mu: mu)
    a = [lower[i, at[0], at[1]] for i in range(12)]
    b = [upper[i, at[0], at[1]] for i in range(12)]
    d = [[b[4 * c + m] - a[4 * c + m] for m in range(4)] for c in range(3)]
    s = [[a[4 * c + m] + b[4 * c + m] if m else None for m in range(4)] for c in range(3)]

    def squares(*values):
        total = None
        for v in values:
            total = v * v if total is None else total + v * v
        return total

    third, ninth = 1.0 / 3.0, 1.0 / 9.0
    corners = squares(d[0][3], d[1][3], d[2][3])
    pairs = ((d[0][1], s[2][3]), (d[0][2], s[1][3]), (d[1][1], d[2][2]))
    singles = (s[0][3], d[1][2], d[2][1])
    lam_part = (
        squares(d[0][0] + s[1][1] + s[2][2])
        + third * squares(*(p + q for p, q in pairs))
        + ninth * corners
    )
    mu_part = (
        2.0 * squares(d[0][0], s[1][1], s[2][2])
        + squares(d[1][0] + s[0][1], d[2][0] + s[0][2], s[2][1] + s[1][2])
        + squares(*(v for pair in pairs for v in pair))
        + third * (squares(*singles) + squares(singles[0] + singles[1] + singles[2]))
        + (4.0 * ninth) * corners
    )
    return lam * lam_part + mu * mu_part


def next_basis(plane, total, step_ref, shift_ref, w_ref, older_ref, out_ref):
    step, shift = step_ref[plane], shift_ref[plane]
    for c in range(3):
        mm, dm, md, dd = (total[4 * c + m] for m in range(4))
        p = (mm - dm) + pltpu.roll(mm + dm, 1, 0)
        q = (md - dd) + pltpu.roll(md + dd, 1, 0)
        force = (p - q) + pltpu.roll(p + q, 1, 1)
        value = step * force + shift * w_ref[c, plane]
        if older_ref is None:
            value = 0.5 * value
        else:
            value = value - older_ref[c, plane]
        out_ref[c, plane] = value


def coefficients(nu):
    half = 0.5

    def gram(i, j):
        return half * (nu[i + j] + nu[abs(i - j)])

    def image(p):
        out = [None] * (len(p) + 1)

        def add(i, value):
            out[i] = value if out[i] is None else out[i] + value

        for k, value in enumerate(p):
            whole, part = SIGMA * value, (0.5 * SIGMA) * value
            add(k, whole)
            if k == 0:
                add(1, whole)
            else:
                add(k + 1, part)
                add(k - 1, part)
        return out

    def form(u, v):
        total = None
        for i, ui in enumerate(u):
            row = None
            for j, vj in enumerate(v):
                term = gram(i, j) * vj
                row = term if row is None else row + term
            total = ui * row if total is None else total + ui * row
        return total

    one = jnp.ones_like(nu[0])
    solution, residual, direction = [], [one], [one]
    descent = gram(0, 0)
    for iteration in range(ITERS):
        moved = image(direction)
        step = descent / form(direction, moved)
        solution = [
            step * p + (solution[k] if k < len(solution) else 0.0) for k, p in enumerate(direction)
        ]
        residual = [
            (residual[k] - step * m) if k < len(residual) else -(step * m)
            for k, m in enumerate(moved)
        ]
        if iteration + 1 < ITERS:
            new = form(residual, residual)
            ratio = new / descent
            direction = [
                r + ratio * direction[k] if k < len(direction) else r
                for k, r in enumerate(residual)
            ]
            descent = new
    return solution, residual


def place(x, y, z, core):
    return {"gx": ((y // 2) * 4 + x) * 2 + core, "gy": lax.rem(y, 2) * 8 + z}


def kernel(r_hbm, l_hbm, w0, w1, w2, w3, w4, diag, factors, r_in, labels, step_ref, shift_ref, below,
           *rest):
    sets, rest = [rest[4 * k : 4 * k + 4] for k in range(3)], rest[12:]
    (from_x, from_y, from_xy, mine, theirs, load_sem, send_sem, recv_sem,
     face_send, face_recv, edge_send, edge_recv, sum_send, sum_recv) = rest
    gx, gy = lax.axis_index("gx"), lax.axis_index("gy")
    core, x, y_hi = lax.rem(gx, 2), lax.rem(gx // 2, 4), gx // 8
    z, y_lo = lax.rem(gy, 8), gy // 8
    y = y_hi * 2 + y_lo

    def neighbour(dx, dy):
        return {"gx": lax.rem(gx + dx + GROUP, GROUP), "gy": lax.rem(gy + dy + GROUP, GROUP)}

    stages = [
        [place(lax.rem(x + k // 4, 4), lax.rem(y + k % 4, 4), z, core) for k in range(1, GROUP)],
        [place(x, y, lax.rem(z + k // 2, 8), lax.rem(core + k % 2, 2)) for k in range(1, GROUP)],
    ]
    barrier = pltpu.get_barrier_semaphore()
    greeted = [neighbour(dx, dy) for dx, dy in DIRECTIONS] + stages[0] + stages[1]
    for device in greeted:
        pl.semaphore_signal(barrier, inc=1, device_id=device, device_id_type=MESH)
    own = (pl.ds(HALO, NX), pl.ds(0, NY))
    load_r = pltpu.make_async_copy(r_hbm, r_in.at[:, own[0], own[1]], load_sem.at[0])
    load_l = pltpu.make_async_copy(l_hbm, labels.at[own[0], own[1]], load_sem.at[1])
    load_r.start()
    load_l.start()
    load_r.wait()
    load_l.wait()
    pl.semaphore_wait(barrier, len(greeted))

    def piece(xs, ys, xd, yd, device, sends, recvs):
        pairs = ((labels.at[xs, ys], labels.at[xd, yd]), (r_in.at[:, xs, ys], r_in.at[:, xd, yd]))
        return [
            pltpu.make_async_remote_copy(
                src_ref=source, dst_ref=target, send_sem=sends(kind), recv_sem=recvs(kind),
                device_id=device, device_id_type=MESH,
            )
            for kind, (source, target) in enumerate(pairs)
        ]

    def rows(dy):
        return (pl.ds({1: 4, 0: 0, -1: 0}[dy], NY if dy == 0 else 4),
                pl.ds({1: 12, 0: 0, -1: 8}[dy], NY if dy == 0 else 4))

    def slab(number):
        dx, dy = DIRECTIONS[number]
        ys, yd = rows(dy)
        return piece(
            pl.ds(NX if dx == 1 else HALO, HALO), ys, pl.ds(0 if dx == 1 else HALO + NX, HALO), yd,
            neighbour(dx, dy),
            lambda kind: send_sem.at[kind, number], lambda kind: recv_sem.at[kind, number],
        )

    def face(part, side):
        ys, yd = rows(1 - 2 * side)
        at = pl.ds(HALO * part, HALO)
        return piece(
            at, ys, at, yd, neighbour(0, 1 - 2 * side),
            lambda kind: face_send.at[kind, side, part - 1],
            lambda kind: face_recv.at[kind, side, part - 1],
        )

    halo = []
    for number in (0, 1, 2):
        halo += slab(number)
    for part in range(1, 5):
        halo += face(part, 0) + face(part, 1)
    for number in (3, 4, 5):
        halo += slab(number)
    for copy in halo:
        copy.start()

    def corner_sums(plane):
        value = pick(labels[plane] > 0, lambda la, mu: (la + 4.0 * mu) / 9.0)
        value = value + pltpu.roll(value, 1, 1)
        return value + pltpu.roll(value, 1, 0)

    def diagonal_plane(plane):
        here = corner_sums(plane)
        value = here + below[...] + KAPPA
        below[...] = here
        inverse = 1.0 / value
        diag[plane] = value
        step = STEP * inverse
        step_ref[plane] = step
        shift_ref[plane] = (RAW * KAPPA) * step - 2.0
        for c in range(3):
            w0[c, plane] = r_in[c, plane] * inverse

    basis = (w0, w1, w2, w3, w4)

    def level(k, plane, parity):
        even, odd, carry, total = sets[k - 1]
        lower, upper = (even, odd) if parity == 0 else (odd, even)
        older = basis[k - 2] if k > 1 else None
        plane_modes(basis[k - 1], plane + 1, upper)
        voxel_forces(plane, labels, lower, upper, carry, total)
        next_basis(plane, total, step_ref, shift_ref, basis[k - 1], older, basis[k])

    for number in (0, 1, 2):
        for copy in slab(number):
            copy.wait_recv()
    below[...] = corner_sums(0)
    for p in range(1, 6):
        if p == 4:
            for side in (0, 1):
                for copy in face(1, side):
                    copy.wait_recv()
        diagonal_plane(p)
        for k in (1, 2, 3):
            if p == 2 * k - 1:
                plane_modes(basis[k - 1], k, sets[k - 1][k % 2])
            elif p >= 2 * k:
                level(k, p - k, (p - k) % 2)

    def two_planes(number, _):
        first = 6 + 2 * number

        @pl.when(lax.rem(first, 4) == 0)
        def _():
            @pl.when(first < HALO + NX)
            def _():
                for side in (0, 1):
                    for copy in face(first // 4, side):
                        copy.wait_recv()

            @pl.when(first == HALO + NX)
            def _():
                for number in (3, 4, 5):
                    for copy in slab(number):
                        copy.wait_recv()

        for extra in (0, 1):
            diagonal_plane(first + extra)
            for k in (1, 2, 3):
                level(k, first + extra - k, (extra - k) % 2)
        return 0

    lax.fori_loop(0, 9, two_planes, 0)

    edges = [
        (w3.at[:, pl.ds(HALO + NX - 1, 1)], from_x, (1, 0)),
        (w3.at[:, pl.ds(HALO, NX + 1), pl.ds(NY - 1, 1)], from_y.at[:, :, pl.ds(NY - 1, 1)], (0, 1)),
        (w3.at[:, pl.ds(HALO + NX - 1, 1), pl.ds(0, NY)], from_xy, (1, 1)),
    ]
    edge_copies = []
    for number, (source, target, (dx, dy)) in enumerate(edges):
        copy = pltpu.make_async_remote_copy(
            src_ref=source, dst_ref=target,
            send_sem=edge_send.at[number], recv_sem=edge_recv.at[number],
            device_id=neighbour(dx, dy), device_id_type=MESH,
        )
        copy.start()
        edge_copies.append(copy)

    zero = jnp.zeros((NY, 128), jnp.float32)
    even, odd, carry, total = sets[0]
    plane_modes(w3, HALO, even)

    def inner(plane, lower, upper, sums):
        sums = list(sums)
        plane_modes(w3, plane + 1, upper)
        for lane in (0, 128):
            at = (slice(0, NY), slice(lane, lane + 128))
            weight = diag[plane, at[0], at[1]]
            for c in range(3):
                w = [ref[c, plane, at[0], at[1]] for ref in basis[:4]]
                scaled = [weight * v for v in w]
                for i, (j, k) in enumerate(DOTS):
                    sums[i] = sums[i] + scaled[j] * w[k]
                sums[7] = sums[7] + (RAW * KAPPA) * (w[3] * w[3])
            sums[7] = sums[7] + voxel_energy(plane, labels, at, lower, upper)
        return tuple(sums)

    def inner_two(number, sums):
        plane = HALO + 2 * number
        sums = inner(plane, even, odd, sums)
        return inner(plane + 1, odd, even, sums)

    sums = lax.fori_loop(0, NX // 2, inner_two, (zero,) * 8)
    lane = lax.broadcasted_iota(jnp.int32, (1, 128), 1)
    row = jnp.zeros((1, 128), jnp.float32)
    for i, value in enumerate(sums):
        value = jnp.sum(jnp.sum(value, axis=0, keepdims=True), axis=1, keepdims=True)
        row = jnp.where(lane == i, value, row)

    def share(stage, row):
        mine[stage] = row
        copies = []
        for number, device in enumerate(stages[stage]):
            copy = pltpu.make_async_remote_copy(
                src_ref=mine.at[stage], dst_ref=theirs.at[stage, number],
                send_sem=sum_send.at[stage, number], recv_sem=sum_recv.at[stage, number],
                device_id=device, device_id_type=MESH,
            )
            copy.start()
            copies.append(copy)
        return copies

    def collect(stage, row, copies):
        for copy in copies:
            copy.wait()
        for number in range(len(copies)):
            row = row + theirs[stage, number]
        return row

    copies = share(0, row)
    for copy in halo:
        copy.wait_send()
    for copy in edge_copies:
        copy.wait()
    for c in range(3):
        w3[c, HALO - 1, 0:8] = from_x[c, 0, 0:8]
        w3[c, HALO - 1, 8:16] = from_x[c, 0, 8:16]
        w3[c, HALO - 1, 15:16] = from_xy[c, 0, 7:8]
        for plane in range(NX + 1):
            w3[c, HALO + plane, 15:16] = from_y[c, plane, 7:8]
    row = collect(0, row, copies)
    copies = share(1, row)

    def last_level(plane, lower, upper):
        plane_modes(w3, plane + 1, upper)
        voxel_forces(plane, labels, lower, upper, carry, total)
        next_basis(plane, total, step_ref, shift_ref, w3, w2, w4)

    def last_two(number, _):
        plane = HALO - 1 + 2 * number
        last_level(plane, even, odd)
        last_level(plane + 1, odd, even)
        return 0

    plane_modes(w3, HALO - 1, even)
    lax.fori_loop(0, NX // 2, last_two, 0)
    last_level(HALO + NX - 1, even, odd)

    row = collect(1, row, copies)
    dots = [
        jnp.sum(jnp.where(lane == i, row, 0.0), axis=1, keepdims=True) for i in range(8)
    ]
    last = (2.0 / (RAW * SIGMA)) * dots[7] - 2.0 * dots[6] - dots[5]
    nu = [
        dots[0], dots[1], 2.0 * dots[2] - dots[0], 2.0 * dots[3] - dots[1],
        2.0 * dots[4] - dots[0], 2.0 * dots[5] - dots[1], 2.0 * dots[6] - dots[0],
        2.0 * last - dots[1],
    ]
    solution, residual = coefficients(nu)
    for k, value in enumerate(solution + residual):
        factors[k] = jnp.broadcast_to(value, (NY, 128))


PART = 4


def combine(w0, w1, w2, w3, w4, diag, factors, sol_hbm, res_hbm, sol, res, sems):
    basis = (w0, w1, w2, w3, w4)
    solution = [factors[k] for k in range(4)]
    residual = [factors[4 + k] for k in range(5)]
    copies = []
    for part in range(NX // PART):
        def one(number, _):
            plane = HALO + number
            for c in range(3):
                for lane in (0, 128):
                    at = (slice(0, NY), slice(lane, lane + 128))
                    w = [ref[c, plane, at[0], at[1]] for ref in basis]
                    x = solution[0] * w[0]
                    r = residual[0] * w[0]
                    for k in range(1, 5):
                        if k < 4:
                            x = x + solution[k] * w[k]
                        r = r + residual[k] * w[k]
                    sol[c, number, at[0], at[1]] = x
                    res[c, number, at[0], at[1]] = diag[plane, at[0], at[1]] * r
            return 0

        lax.fori_loop(part * PART, part * PART + PART, one, 0)
        planes = pl.ds(part * PART, PART)
        for i, (source, target) in enumerate(((sol, sol_hbm), (res, res_hbm))):
            copy = pltpu.make_async_copy(source.at[:, planes], target.at[:, planes], sems.at[i, part])
            copy.start()
            copies.append(copy)
    for copy in copies:
        copy.wait()


def local(right_side, labels):
    shape = (3, NX, NY, NZ)
    wide = jax.ShapeDtypeStruct((3, PX, PY, NZ), jnp.float32)
    vector = pltpu.VMEM((3, PX, PY, NZ), jnp.float32)
    in_vmem = pl.BlockSpec(memory_space=pltpu.VMEM)
    in_hbm = pl.BlockSpec(memory_space=pltpu.HBM)
    scalar = pltpu.VMEM((PX, PY, NZ), jnp.float32)
    modes = pltpu.VMEM((12, PY, NZ), jnp.float32)
    parts = pl.pallas_call(
        kernel,
        out_shape=(*([wide] * 5), jax.ShapeDtypeStruct((PX, PY, NZ), jnp.float32),
                   jax.ShapeDtypeStruct((9, NY, 128), jnp.float32)),
        in_specs=[in_hbm] * 2,
        out_specs=[in_vmem] * 7,
        scratch_shapes=[
            vector, pltpu.VMEM((PX, PY, NZ), jnp.int32), scalar, scalar,
            pltpu.VMEM((PY, NZ), jnp.float32),
            *([modes] * 12),
            pltpu.VMEM((3, 1, PY, NZ), jnp.float32),
            pltpu.VMEM((3, NX + 1, NY, NZ), jnp.float32),
            pltpu.VMEM((3, 1, NY, NZ), jnp.float32),
            pltpu.VMEM((2, 1, 128), jnp.float32),
            pltpu.VMEM((2, GROUP - 1, 1, 128), jnp.float32),
            pltpu.SemaphoreType.DMA((2,)),
            pltpu.SemaphoreType.DMA((2, 6)),
            pltpu.SemaphoreType.DMA((2, 6)),
            pltpu.SemaphoreType.DMA((2, 2, 4)),
            pltpu.SemaphoreType.DMA((2, 2, 4)),
            pltpu.SemaphoreType.DMA((3,)),
            pltpu.SemaphoreType.DMA((3,)),
            pltpu.SemaphoreType.DMA((2, GROUP - 1)),
            pltpu.SemaphoreType.DMA((2, GROUP - 1)),
        ],
        compiler_params=pltpu.CompilerParams(
            collective_id=0, has_side_effects=True, vmem_limit_bytes=24 * 1024 * 1024
        ),
    )(*(pltpu.with_memory_space_constraint(a, pltpu.HBM) for a in (right_side, labels)))
    block = pltpu.VMEM(shape, jnp.float32)
    return pl.pallas_call(
        combine,
        out_shape=(jax.ShapeDtypeStruct(shape, jnp.float32),) * 2,
        in_specs=[in_vmem] * 7,
        out_specs=[in_hbm] * 2,
        scratch_shapes=[block, block, pltpu.SemaphoreType.DMA((2, NX // PART))],
        compiler_params=pltpu.CompilerParams(vmem_limit_bytes=8 * 1024 * 1024),
    )(*parts)


def solution(mesh):
    specs = P(None, "gx", "gy", None)
    return jax.shard_map(
        local, mesh=mesh, in_specs=(specs, P("gx", "gy", None)), out_specs=(specs, specs),
        check_vma=False,
    )
```

```python
import jax
import jax.numpy as jnp
from jax import lax
from jax.experimental import pallas as pl
from jax.experimental.pallas import tpu as pltpu
from jax.sharding import PartitionSpec as P

MESH = pl.DeviceIdType.MESH
ITERS = 4
LAMBDA_SOFT = 0.5769231
LAMBDA_RISE = 1.6452991
SHEAR_SOFT = 0.3846154
SHEAR_RISE = 2.9487179
KAPPA = 0.05

NX, NY, NZ = 16, 8, 256
HALO = 4
PX = NX + 2 * HALO
PY = 16
GROUP = 16
SIGMA = 1.05
RAW = 16.0
STEP = 2.0 / (RAW * SIGMA)

DIRECTIONS = [(1, 0), (1, 1), (1, -1), (-1, 0), (-1, 1), (-1, -1), (0, 1), (0, -1)]
DOTS = [(0, 0), (0, 1), (1, 1), (1, 2), (2, 2), (2, 3), (3, 3)]


def phases(form):
    soft = form(LAMBDA_SOFT, SHEAR_SOFT)
    stiff = form(LAMBDA_SOFT + LAMBDA_RISE, SHEAR_SOFT + SHEAR_RISE)
    return soft, stiff


def pick(stiff_mask, form):
    soft, stiff = phases(form)
    return jnp.where(stiff_mask, jnp.float32(stiff), jnp.float32(soft))


TILES = ((0, 0), (0, 1), (1, 0), (1, 1))


def tile(t):
    row, half = t
    return slice(8 * row, 8 * row + 8), slice(128 * half, 128 * half + 128)


def along_z(pair, shift):
    edge = 127 if shift < 0 else 0
    at_edge = lax.broadcasted_iota(jnp.int32, (8, 128), 1) == edge
    low, high = (pltpu.roll(v, shift % 128, 1) for v in pair)
    return jnp.where(at_edge, high, low), jnp.where(at_edge, low, high)


def along_y(pair, shift):
    edge = 7 if shift < 0 else 0
    at_edge = lax.broadcasted_iota(jnp.int32, (8, 128), 0) == edge
    low, high = (pltpu.roll(v, shift % 8, 0) for v in pair)
    return jnp.where(at_edge, high, low), jnp.where(at_edge, low, high)


def plane_modes(w_ref, plane, modes, tiles=TILES):
    for c in range(3):
        flat = {}
        for row in (0, 1):
            u = [w_ref[(c, plane, *tile((row, half)))] for half in (0, 1)]
            uz = along_z(u, -1)
            for half in (0, 1):
                flat[row, half] = (u[half] + uz[half], uz[half] - u[half])
        for kind in (0, 1):
            for half in (0, 1):
                value = [flat[row, half][kind] for row in (0, 1)]
                above = along_y(value, -1)
                for row in (0, 1):
                    if (row, half) in tiles:
                        at = tile((row, half))
                        modes[4 * c + 2 * kind, at[0], at[1]] = value[row] + above[row]
                        modes[4 * c + 2 * kind + 1, at[0], at[1]] = above[row] - value[row]


def voxel_forces(plane, label_ref, lower, upper, carry, level):
    for row, half in TILES:
        at = tile((row, half))
        stiff = label_ref[plane, at[0], at[1]] > 0
        lam = pick(stiff, lambda la, mu: la)
        mu = pick(stiff, lambda la, mu: mu)
        mu2 = pick(stiff, lambda la, mu: 2.0 * mu)
        lam3 = pick(stiff, lambda la, mu: la / 3.0)
        mu3 = pick(stiff, lambda la, mu: mu / 3.0)
        dd9 = pick(stiff, lambda la, mu: (la + 4.0 * mu) / 9.0)
        a = [lower[i, at[0], at[1]] for i in range(12)]
        b = [upper[i, at[0], at[1]] for i in range(12)]
        d = [[b[4 * c + m] - a[4 * c + m] for m in range(4)] for c in range(3)]
        s = [[a[4 * c + m] + b[4 * c + m] if m else None for m in range(4)] for c in range(3)]
        fd = [[None] * 4 for _ in range(3)]
        fs = [[None] * 4 for _ in range(3)]
        trace = lam * (d[0][0] + s[1][1] + s[2][2])
        fd[0][0] = trace + mu2 * d[0][0]
        fs[1][1] = trace + mu2 * s[1][1]
        fs[2][2] = trace + mu2 * s[2][2]
        fd[1][0] = fs[0][1] = mu * (d[1][0] + s[0][1])
        fd[2][0] = fs[0][2] = mu * (d[2][0] + s[0][2])
        fs[2][1] = fs[1][2] = mu * (s[2][1] + s[1][2])
        h = lam3 * (d[0][1] + s[2][3])
        fd[0][1], fs[2][3] = h + mu * d[0][1], h + mu * s[2][3]
        h = lam3 * (d[0][2] + s[1][3])
        fd[0][2], fs[1][3] = h + mu * d[0][2], h + mu * s[1][3]
        h = lam3 * (d[1][1] + d[2][2])
        fd[1][1], fd[2][2] = h + mu * d[1][1], h + mu * d[2][2]
        three = s[0][3] + d[1][2] + d[2][1]
        fs[0][3] = mu3 * (s[0][3] + three)
        fd[1][2] = mu3 * (d[1][2] + three)
        fd[2][1] = mu3 * (d[2][1] + three)
        for c in range(3):
            fd[c][3] = dd9 * d[c][3]
        for c in range(3):
            node = []
            for m in range(4):
                i = 4 * c + m
                before = carry[i, at[0], at[1]]
                if m == 0:
                    node.append(before - fd[c][0])
                    carry[i, at[0], at[1]] = fd[c][0]
                else:
                    node.append(before + (fs[c][m] - fd[c][m]))
                    carry[i, at[0], at[1]] = fs[c][m] + fd[c][m]
            for kind in (0, 1):
                m, d_ = node[2 * kind], node[2 * kind + 1]
                level[2 * c + kind, at[0], at[1]] = m - d_
                level[6 + 2 * c + kind, at[0], at[1]] = m + d_


def voxel_energy(plane, label_ref, at, lower, upper):
    stiff = label_ref[plane, at[0], at[1]] > 0
    lam = pick(stiff, lambda la, mu: la)
    mu = pick(stiff, lambda la, mu: mu)
    a = [lower[i, at[0], at[1]] for i in range(12)]
    b = [upper[i, at[0], at[1]] for i in range(12)]
    d = [[b[4 * c + m] - a[4 * c + m] for m in range(4)] for c in range(3)]
    s = [[a[4 * c + m] + b[4 * c + m] if m else None for m in range(4)] for c in range(3)]

    def squares(*values):
        total = None
        for v in values:
            total = v * v if total is None else total + v * v
        return total

    third, ninth = 1.0 / 3.0, 1.0 / 9.0
    corners = squares(d[0][3], d[1][3], d[2][3])
    pairs = ((d[0][1], s[2][3]), (d[0][2], s[1][3]), (d[1][1], d[2][2]))
    singles = (s[0][3], d[1][2], d[2][1])
    lam_part = (
        squares(d[0][0] + s[1][1] + s[2][2])
        + third * squares(*(p + q for p, q in pairs))
        + ninth * corners
    )
    mu_part = (
        2.0 * squares(d[0][0], s[1][1], s[2][2])
        + squares(d[1][0] + s[0][1], d[2][0] + s[0][2], s[2][1] + s[1][2])
        + squares(*(v for pair in pairs for v in pair))
        + third * (squares(*singles) + squares(singles[0] + singles[1] + singles[2]))
        + (4.0 * ninth) * corners
    )
    return lam * lam_part + mu * mu_part


def next_basis(plane, level, step_ref, shift_ref, w_ref, older_ref, out_ref, rows=(0, 1)):
    for c in range(3):
        sums = {}
        for half in (0, 1):
            for kind in (0, 1):
                at = [tile((row, half)) for row in (0, 1)]
                moved = along_y([level[(6 + 2 * c + kind, *at[row])] for row in (0, 1)], 1)
                for row in rows:
                    sums[row, half, kind] = level[(2 * c + kind, *at[row])] + moved[row]
        for row in rows:
            upper = along_z([sums[row, half, 0] + sums[row, half, 1] for half in (0, 1)], 1)
            for half in (0, 1):
                at = tile((row, half))
                force = (sums[row, half, 0] - sums[row, half, 1]) + upper[half]
                value = step_ref[(plane, *at)] * force + shift_ref[(plane, *at)] * w_ref[(c, plane, *at)]
                if older_ref is None:
                    value = 0.5 * value
                else:
                    value = value - older_ref[(c, plane, *at)]
                out_ref[(c, plane, *at)] = value


def coefficients(nu):
    half = 0.5

    def gram(i, j):
        return half * (nu[i + j] + nu[abs(i - j)])

    def image(p):
        out = [None] * (len(p) + 1)

        def add(i, value):
            out[i] = value if out[i] is None else out[i] + value

        for k, value in enumerate(p):
            whole, part = SIGMA * value, (0.5 * SIGMA) * value
            add(k, whole)
            if k == 0:
                add(1, whole)
            else:
                add(k + 1, part)
                add(k - 1, part)
        return out

    def form(u, v):
        total = None
        for i, ui in enumerate(u):
            row = None
            for j, vj in enumerate(v):
                term = gram(i, j) * vj
                row = term if row is None else row + term
            total = ui * row if total is None else total + ui * row
        return total

    one = jnp.ones_like(nu[0])
    solution, residual, direction = [], [one], [one]
    descent = gram(0, 0)
    for iteration in range(ITERS):
        moved = image(direction)
        step = descent / form(direction, moved)
        solution = [
            step * p + (solution[k] if k < len(solution) else 0.0) for k, p in enumerate(direction)
        ]
        residual = [
            (residual[k] - step * m) if k < len(residual) else -(step * m)
            for k, m in enumerate(moved)
        ]
        if iteration + 1 < ITERS:
            new = form(residual, residual)
            ratio = new / descent
            direction = [
                r + ratio * direction[k] if k < len(direction) else r
                for k, r in enumerate(residual)
            ]
            descent = new
    return solution, residual


def place(x, y, z, core):
    return {"gx": ((y // 2) * 4 + x) * 2 + core, "gy": lax.rem(y, 2) * 8 + z}


def kernel(r_hbm, l_hbm, w0, w1, w2, w3, w4, diag, factors, r_in, labels, step_ref, shift_ref, below,
           *rest):
    sets, rest = [rest[5 * k : 5 * k + 5] for k in range(3)], rest[15:]
    (from_x, from_y, from_xy, mine, theirs, load_sem, send_sem, recv_sem,
     face_send, face_recv, edge_send, edge_recv, sum_send, sum_recv) = rest
    gx, gy = lax.axis_index("gx"), lax.axis_index("gy")
    core, x, y_hi = lax.rem(gx, 2), lax.rem(gx // 2, 4), gx // 8
    z, y_lo = lax.rem(gy, 8), gy // 8
    y = y_hi * 2 + y_lo

    def neighbour(dx, dy):
        return {"gx": lax.rem(gx + dx + GROUP, GROUP), "gy": lax.rem(gy + dy + GROUP, GROUP)}

    stages = [
        [place(lax.rem(x + k // 4, 4), lax.rem(y + k % 4, 4), z, core) for k in range(1, GROUP)],
        [place(x, y, lax.rem(z + k // 2, 8), lax.rem(core + k % 2, 2)) for k in range(1, GROUP)],
    ]
    barrier = pltpu.get_barrier_semaphore()
    greeted = [neighbour(dx, dy) for dx, dy in DIRECTIONS] + stages[0] + stages[1]
    for device in greeted:
        pl.semaphore_signal(barrier, inc=1, device_id=device, device_id_type=MESH)
    own = (pl.ds(HALO, NX), pl.ds(0, NY))
    load_r = pltpu.make_async_copy(r_hbm, r_in.at[:, own[0], own[1]], load_sem.at[0])
    load_l = pltpu.make_async_copy(l_hbm, labels.at[own[0], own[1]], load_sem.at[1])
    load_r.start()
    load_l.start()
    load_r.wait()
    load_l.wait()
    pl.semaphore_wait(barrier, len(greeted))

    def piece(xs, ys, xd, yd, device, sends, recvs):
        pairs = ((labels.at[xs, ys], labels.at[xd, yd]), (r_in.at[:, xs, ys], r_in.at[:, xd, yd]))
        return [
            pltpu.make_async_remote_copy(
                src_ref=source, dst_ref=target, send_sem=sends(kind), recv_sem=recvs(kind),
                device_id=device, device_id_type=MESH,
            )
            for kind, (source, target) in enumerate(pairs)
        ]

    def rows(dy):
        return (pl.ds({1: 4, 0: 0, -1: 0}[dy], NY if dy == 0 else 4),
                pl.ds({1: 12, 0: 0, -1: 8}[dy], NY if dy == 0 else 4))

    def slab(number):
        dx, dy = DIRECTIONS[number]
        ys, yd = rows(dy)
        return piece(
            pl.ds(NX if dx == 1 else HALO, HALO), ys, pl.ds(0 if dx == 1 else HALO + NX, HALO), yd,
            neighbour(dx, dy),
            lambda kind: send_sem.at[kind, number], lambda kind: recv_sem.at[kind, number],
        )

    def face(part, side):
        ys, yd = rows(1 - 2 * side)
        at = pl.ds(2 * part + 2, 2)
        return piece(
            at, ys, at, yd, neighbour(0, 1 - 2 * side),
            lambda kind: face_send.at[kind, side, part - 1],
            lambda kind: face_recv.at[kind, side, part - 1],
        )

    halo = []
    for number in (0, 1, 2):
        halo += slab(number)
    for part in range(1, 9):
        halo += face(part, 0) + face(part, 1)
    for number in (3, 4, 5):
        halo += slab(number)
    for copy in halo:
        copy.start()

    def corner_sums(plane):
        value = pick(labels[plane] > 0, lambda la, mu: (la + 4.0 * mu) / 9.0)
        value = value + pltpu.roll(value, 1, 1)
        return value + pltpu.roll(value, 1, 0)

    def diagonal_plane(plane):
        here = corner_sums(plane)
        value = here + below[...] + KAPPA
        below[...] = here
        inverse = 1.0 / value
        diag[plane] = value
        step = STEP * inverse
        step_ref[plane] = step
        shift_ref[plane] = (RAW * KAPPA) * step - 2.0
        for c in range(3):
            w0[c, plane] = r_in[c, plane] * inverse

    basis = (w0, w1, w2, w3, w4)

    def modes_of(k, plane, parity, tiles=TILES, ref=None):
        ref = basis[k - 1] if ref is None else ref
        plane_modes(ref, plane, sets[k - 1][parity], tiles)

    def forces_of(k, plane, parity):
        group = sets[k - 1]
        voxel_forces(plane, labels, group[parity], group[1 - parity], group[4],
                     group[2 + parity])

    def next_of(k, plane, parity):
        group, older = sets[k - 1], basis[k - 2] if k > 1 else None
        next_basis(plane, group[2 + parity], step_ref, shift_ref,
                   basis[k - 1], older, basis[k])

    def level(k, plane, parity, count):
        for i in range(count):
            modes_of(k, plane + i + 1, (parity + i + 1) % 2)
            forces_of(k, plane + i, (parity + i) % 2)
        for i in range(count):
            next_of(k, plane + i, (parity + i) % 2)

    def arrived(copies):
        for copy in copies:
            copy.wait_recv()

    def levels(first, which):
        for k in which:
            level(k, first - 3 * k, k % 2, 2)

    def diagonals(first):
        for extra in (0, 1):
            diagonal_plane(first + extra)

    below[...] = jnp.zeros_like(below)
    arrived(slab(0) + slab(1) + slab(2))
    diagonals(0)
    diagonals(2)
    modes_of(1, 1, 1)
    levels(4, (1,))
    arrived(face(1, 0) + face(1, 1))
    diagonals(4)
    modes_of(2, 2, 0)
    levels(6, (1,))
    arrived(face(2, 0) + face(2, 1))
    diagonals(6)
    levels(8, (2, 1))
    arrived(face(3, 0) + face(3, 1))
    diagonals(8)
    modes_of(3, 3, 1)
    levels(10, (2, 1))
    arrived(face(4, 0) + face(4, 1))
    diagonals(10)

    def steady(number, _):
        first = 12 + 2 * number

        @pl.when(first < HALO + NX)
        def _():
            part = first // 2 - 1
            arrived(face(part, 0) + face(part, 1))

        @pl.when(first == HALO + NX)
        def _():
            arrived(slab(3) + slab(4) + slab(5))

        levels(first, (3, 2, 1))
        diagonals(first)
        return 0

    lax.fori_loop(0, 6, steady, 0)
    levels(24, (3, 2, 1))
    levels(26, (3, 2))
    levels(28, (3,))

    edges = [
        (w3.at[:, pl.ds(HALO + NX - 1, 1)], from_x, (1, 0)),
        (w3.at[:, pl.ds(HALO, NX + 1), pl.ds(NY - 1, 1)], from_y.at[:, :, pl.ds(NY - 1, 1)], (0, 1)),
        (w3.at[:, pl.ds(HALO + NX - 1, 1), pl.ds(0, NY)], from_xy, (1, 1)),
    ]
    edge_copies = []
    for number, (source, target, (dx, dy)) in enumerate(edges):
        copy = pltpu.make_async_remote_copy(
            src_ref=source, dst_ref=target,
            send_sem=edge_send.at[number], recv_sem=edge_recv.at[number],
            device_id=neighbour(dx, dy), device_id_type=MESH,
        )
        copy.start()
        edge_copies.append(copy)

    zero = jnp.zeros((NY, 128), jnp.float32)
    near = TILES[:2]
    modes_of(1, HALO, 0, near, w3)

    def inner(plane, parity, sums):
        sums = list(sums)
        modes_of(1, plane + 1, 1 - parity, near, w3)
        lower, upper = sets[0][parity], sets[0][1 - parity]
        for lane in (0, 128):
            at = (slice(0, NY), slice(lane, lane + 128))
            weight = diag[plane, at[0], at[1]]
            for c in range(3):
                w = [ref[c, plane, at[0], at[1]] for ref in basis[:4]]
                scaled = [weight * v for v in w]
                for i, (j, k) in enumerate(DOTS):
                    sums[i] = sums[i] + scaled[j] * w[k]
                sums[7] = sums[7] + (RAW * KAPPA) * (w[3] * w[3])
            sums[7] = sums[7] + voxel_energy(plane, labels, at, lower, upper)
        return tuple(sums)

    def inner_two(number, sums):
        plane = HALO + 2 * number
        sums = inner(plane, 0, sums)
        return inner(plane + 1, 1, sums)

    sums = lax.fori_loop(0, NX // 2, inner_two, (zero,) * 8)
    lane = lax.broadcasted_iota(jnp.int32, (1, 128), 1)
    row = jnp.zeros((1, 128), jnp.float32)
    for i, value in enumerate(sums):
        value = jnp.sum(jnp.sum(value, axis=0, keepdims=True), axis=1, keepdims=True)
        row = jnp.where(lane == i, value, row)

    def share(stage, row):
        mine[stage] = row
        copies = []
        for number, device in enumerate(stages[stage]):
            copy = pltpu.make_async_remote_copy(
                src_ref=mine.at[stage], dst_ref=theirs.at[stage, number],
                send_sem=sum_send.at[stage, number], recv_sem=sum_recv.at[stage, number],
                device_id=device, device_id_type=MESH,
            )
            copy.start()
            copies.append(copy)
        return copies

    def collect(stage, row, copies):
        for copy in copies:
            copy.wait()
        for number in range(len(copies)):
            row = row + theirs[stage, number]
        return row

    copies = share(0, row)
    for copy in halo:
        copy.wait_send()
    for copy in edge_copies:
        copy.wait()
    for c in range(3):
        w3[c, HALO - 1, 0:8] = from_x[c, 0, 0:8]
        w3[c, HALO - 1, 8:16] = from_x[c, 0, 8:16]
        w3[c, HALO - 1, 15:16] = from_xy[c, 0, 7:8]
        for plane in range(NX + 1):
            w3[c, HALO + plane, 15:16] = from_y[c, plane, 7:8]
    row = collect(0, row, copies)
    copies = share(1, row)

    def last_level(plane, parity):
        modes_of(1, plane + 1, 1 - parity, TILES, w3)
        forces_of(1, plane, parity)
        next_basis(plane, sets[0][2 + parity], step_ref, shift_ref,
                   w3, w2, w4, (0,))

    def last_two(number, _):
        plane = HALO - 1 + 2 * number
        last_level(plane, 1)
        last_level(plane + 1, 0)
        return 0

    modes_of(1, HALO - 1, 1, TILES, w3)
    lax.fori_loop(0, NX // 2, last_two, 0)
    last_level(HALO + NX - 1, 1)

    row = collect(1, row, copies)
    dots = [
        jnp.sum(jnp.where(lane == i, row, 0.0), axis=1, keepdims=True) for i in range(8)
    ]
    last = (2.0 / (RAW * SIGMA)) * dots[7] - 2.0 * dots[6] - dots[5]
    nu = [
        dots[0], dots[1], 2.0 * dots[2] - dots[0], 2.0 * dots[3] - dots[1],
        2.0 * dots[4] - dots[0], 2.0 * dots[5] - dots[1], 2.0 * dots[6] - dots[0],
        2.0 * last - dots[1],
    ]
    solution, residual = coefficients(nu)
    for k, value in enumerate(solution + residual):
        factors[k] = jnp.broadcast_to(value, (NY, 128))


PART = 4


def combine(w0, w1, w2, w3, w4, diag, factors, sol_hbm, res_hbm, sol, res, sems):
    basis = (w0, w1, w2, w3, w4)
    solution = [factors[k] for k in range(4)]
    residual = [factors[4 + k] for k in range(5)]
    copies = []
    for part in range(NX // PART):
        def one(number, _):
            plane = HALO + number
            for c in range(3):
                for lane in (0, 128):
                    at = (slice(0, NY), slice(lane, lane + 128))
                    w = [ref[c, plane, at[0], at[1]] for ref in basis]
                    x = solution[0] * w[0]
                    r = residual[0] * w[0]
                    for k in range(1, 5):
                        if k < 4:
                            x = x + solution[k] * w[k]
                        r = r + residual[k] * w[k]
                    sol[c, number, at[0], at[1]] = x
                    res[c, number, at[0], at[1]] = diag[plane, at[0], at[1]] * r
            return 0

        lax.fori_loop(part * PART, part * PART + PART, one, 0)
        planes = pl.ds(part * PART, PART)
        for i, (source, target) in enumerate(((sol, sol_hbm), (res, res_hbm))):
            copy = pltpu.make_async_copy(source.at[:, planes], target.at[:, planes], sems.at[i, part])
            copy.start()
            copies.append(copy)
    for copy in copies:
        copy.wait()


def local(right_side, labels):
    shape = (3, NX, NY, NZ)
    wide = jax.ShapeDtypeStruct((3, PX, PY, NZ), jnp.float32)
    vector = pltpu.VMEM((3, PX, PY, NZ), jnp.float32)
    in_vmem = pl.BlockSpec(memory_space=pltpu.VMEM)
    in_hbm = pl.BlockSpec(memory_space=pltpu.HBM)
    scalar = pltpu.VMEM((PX, PY, NZ), jnp.float32)
    modes = pltpu.VMEM((12, PY, NZ), jnp.float32)
    parts = pl.pallas_call(
        kernel,
        out_shape=(*([wide] * 5), jax.ShapeDtypeStruct((PX, PY, NZ), jnp.float32),
                   jax.ShapeDtypeStruct((9, NY, 128), jnp.float32)),
        in_specs=[in_hbm] * 2,
        out_specs=[in_vmem] * 7,
        scratch_shapes=[
            vector, pltpu.VMEM((PX, PY, NZ), jnp.int32), scalar, scalar,
            pltpu.VMEM((PY, NZ), jnp.float32),
            *([modes] * 15),
            pltpu.VMEM((3, 1, PY, NZ), jnp.float32),
            pltpu.VMEM((3, NX + 1, NY, NZ), jnp.float32),
            pltpu.VMEM((3, 1, NY, NZ), jnp.float32),
            pltpu.VMEM((2, 1, 128), jnp.float32),
            pltpu.VMEM((2, GROUP - 1, 1, 128), jnp.float32),
            pltpu.SemaphoreType.DMA((2,)),
            pltpu.SemaphoreType.DMA((2, 6)),
            pltpu.SemaphoreType.DMA((2, 6)),
            pltpu.SemaphoreType.DMA((2, 2, 8)),
            pltpu.SemaphoreType.DMA((2, 2, 8)),
            pltpu.SemaphoreType.DMA((3,)),
            pltpu.SemaphoreType.DMA((3,)),
            pltpu.SemaphoreType.DMA((2, GROUP - 1)),
            pltpu.SemaphoreType.DMA((2, GROUP - 1)),
        ],
        compiler_params=pltpu.CompilerParams(
            collective_id=0, has_side_effects=True, vmem_limit_bytes=24 * 1024 * 1024
        ),
    )(*(pltpu.with_memory_space_constraint(a, pltpu.HBM) for a in (right_side, labels)))
    block = pltpu.VMEM(shape, jnp.float32)
    return pl.pallas_call(
        combine,
        out_shape=(jax.ShapeDtypeStruct(shape, jnp.float32),) * 2,
        in_specs=[in_vmem] * 7,
        out_specs=[in_hbm] * 2,
        scratch_shapes=[block, block, pltpu.SemaphoreType.DMA((2, NX // PART))],
        compiler_params=pltpu.CompilerParams(vmem_limit_bytes=8 * 1024 * 1024),
    )(*parts)


def solution(mesh):
    specs = P(None, "gx", "gy", None)
    return jax.shard_map(
        local, mesh=mesh, in_specs=(specs, P("gx", "gy", None)), out_specs=(specs, specs),
        check_vma=False,
    )
```

```python
import jax
import jax.numpy as jnp
from jax import lax
from jax.experimental import pallas as pl
from jax.experimental.pallas import tpu as pltpu
from jax.sharding import PartitionSpec as P

MESH = pl.DeviceIdType.MESH
ITERS = 4
LAMBDA_SOFT = 0.5769231
LAMBDA_RISE = 1.6452991
SHEAR_SOFT = 0.3846154
SHEAR_RISE = 2.9487179
KAPPA = 0.05

NX, NY, NZ = 16, 8, 256
HALO = 4
PX = NX + 2 * HALO
PY = 16
GROUP = 16
SIGMA = 1.05
RAW = 16.0
STEP = 2.0 / (RAW * SIGMA)

DIRECTIONS = [(1, 0), (1, 1), (1, -1), (-1, 0), (-1, 1), (-1, -1), (0, 1), (0, -1)]
DOTS = [(0, 0), (0, 1), (1, 1), (1, 2), (2, 2), (2, 3), (3, 3)]


def phases(form):
    soft = form(LAMBDA_SOFT, SHEAR_SOFT)
    stiff = form(LAMBDA_SOFT + LAMBDA_RISE, SHEAR_SOFT + SHEAR_RISE)
    return soft, stiff


def pick(stiff_mask, form):
    soft, stiff = phases(form)
    return jnp.where(stiff_mask, jnp.float32(stiff), jnp.float32(soft))


TILES = ((0, 0), (0, 1), (1, 0), (1, 1))


def tile(t):
    row, half = t
    return slice(8 * row, 8 * row + 8), slice(128 * half, 128 * half + 128)


def along_z(pair, shift):
    edge = 127 if shift < 0 else 0
    at_edge = lax.broadcasted_iota(jnp.int32, (8, 128), 1) == edge
    low, high = (pltpu.roll(v, shift % 128, 1) for v in pair)
    return jnp.where(at_edge, high, low), jnp.where(at_edge, low, high)


def along_y(pair, shift):
    edge = 7 if shift < 0 else 0
    at_edge = lax.broadcasted_iota(jnp.int32, (8, 128), 0) == edge
    low, high = (pltpu.roll(v, shift % 8, 0) for v in pair)
    return jnp.where(at_edge, high, low), jnp.where(at_edge, low, high)


def plane_modes(w_ref, plane, modes, tiles=TILES):
    for c in range(3):
        flat = {}
        for row in (0, 1):
            u = [w_ref[(c, plane, *tile((row, half)))] for half in (0, 1)]
            uz = along_z(u, -1)
            for half in (0, 1):
                flat[row, half] = (u[half] + uz[half], uz[half] - u[half])
        for kind in (0, 1):
            for half in (0, 1):
                value = [flat[row, half][kind] for row in (0, 1)]
                above = along_y(value, -1)
                for row in (0, 1):
                    if (row, half) in tiles:
                        at = tile((row, half))
                        modes[4 * c + 2 * kind, at[0], at[1]] = value[row] + above[row]
                        modes[4 * c + 2 * kind + 1, at[0], at[1]] = above[row] - value[row]


def voxel_forces(plane, label_ref, lower, upper, carry, level):
    for row, half in TILES:
        at = tile((row, half))
        stiff = label_ref[plane, at[0], at[1]] > 0
        lam = pick(stiff, lambda la, mu: la)
        mu = pick(stiff, lambda la, mu: mu)
        mu2 = pick(stiff, lambda la, mu: 2.0 * mu)
        lam3 = pick(stiff, lambda la, mu: la / 3.0)
        mu3 = pick(stiff, lambda la, mu: mu / 3.0)
        dd9 = pick(stiff, lambda la, mu: (la + 4.0 * mu) / 9.0)
        a = [lower[i, at[0], at[1]] for i in range(12)]
        b = [upper[i, at[0], at[1]] for i in range(12)]
        d = [[b[4 * c + m] - a[4 * c + m] for m in range(4)] for c in range(3)]
        s = [[a[4 * c + m] + b[4 * c + m] if m else None for m in range(4)] for c in range(3)]
        fd = [[None] * 4 for _ in range(3)]
        fs = [[None] * 4 for _ in range(3)]
        trace = lam * (d[0][0] + s[1][1] + s[2][2])
        fd[0][0] = trace + mu2 * d[0][0]
        fs[1][1] = trace + mu2 * s[1][1]
        fs[2][2] = trace + mu2 * s[2][2]
        fd[1][0] = fs[0][1] = mu * (d[1][0] + s[0][1])
        fd[2][0] = fs[0][2] = mu * (d[2][0] + s[0][2])
        fs[2][1] = fs[1][2] = mu * (s[2][1] + s[1][2])
        h = lam3 * (d[0][1] + s[2][3])
        fd[0][1], fs[2][3] = h + mu * d[0][1], h + mu * s[2][3]
        h = lam3 * (d[0][2] + s[1][3])
        fd[0][2], fs[1][3] = h + mu * d[0][2], h + mu * s[1][3]
        h = lam3 * (d[1][1] + d[2][2])
        fd[1][1], fd[2][2] = h + mu * d[1][1], h + mu * d[2][2]
        three = s[0][3] + d[1][2] + d[2][1]
        fs[0][3] = mu3 * (s[0][3] + three)
        fd[1][2] = mu3 * (d[1][2] + three)
        fd[2][1] = mu3 * (d[2][1] + three)
        for c in range(3):
            fd[c][3] = dd9 * d[c][3]
        for c in range(3):
            node = []
            for m in range(4):
                i = 4 * c + m
                before = carry[i, at[0], at[1]]
                if m == 0:
                    node.append(before - fd[c][0])
                    carry[i, at[0], at[1]] = fd[c][0]
                else:
                    node.append(before + (fs[c][m] - fd[c][m]))
                    carry[i, at[0], at[1]] = fs[c][m] + fd[c][m]
            for kind in (0, 1):
                m, d_ = node[2 * kind], node[2 * kind + 1]
                level[2 * c + kind, at[0], at[1]] = m - d_
                level[6 + 2 * c + kind, at[0], at[1]] = m + d_


def voxel_energy(plane, label_ref, at, lower, upper):
    stiff = label_ref[plane, at[0], at[1]] > 0
    lam = pick(stiff, lambda la, mu: la)
    mu = pick(stiff, lambda la, mu: mu)
    a = [lower[i, at[0], at[1]] for i in range(12)]
    b = [upper[i, at[0], at[1]] for i in range(12)]
    d = [[b[4 * c + m] - a[4 * c + m] for m in range(4)] for c in range(3)]
    s = [[a[4 * c + m] + b[4 * c + m] if m else None for m in range(4)] for c in range(3)]

    def squares(*values):
        total = None
        for v in values:
            total = v * v if total is None else total + v * v
        return total

    third, ninth = 1.0 / 3.0, 1.0 / 9.0
    corners = squares(d[0][3], d[1][3], d[2][3])
    pairs = ((d[0][1], s[2][3]), (d[0][2], s[1][3]), (d[1][1], d[2][2]))
    singles = (s[0][3], d[1][2], d[2][1])
    lam_part = (
        squares(d[0][0] + s[1][1] + s[2][2])
        + third * squares(*(p + q for p, q in pairs))
        + ninth * corners
    )
    mu_part = (
        2.0 * squares(d[0][0], s[1][1], s[2][2])
        + squares(d[1][0] + s[0][1], d[2][0] + s[0][2], s[2][1] + s[1][2])
        + squares(*(v for pair in pairs for v in pair))
        + third * (squares(*singles) + squares(singles[0] + singles[1] + singles[2]))
        + (4.0 * ninth) * corners
    )
    return lam * lam_part + mu * mu_part


def next_basis(plane, level, step_ref, shift_ref, w_ref, older_ref, out_ref, rows=(0, 1)):
    for c in range(3):
        sums = {}
        for half in (0, 1):
            for kind in (0, 1):
                at = [tile((row, half)) for row in (0, 1)]
                moved = along_y([level[(6 + 2 * c + kind, *at[row])] for row in (0, 1)], 1)
                for row in rows:
                    sums[row, half, kind] = level[(2 * c + kind, *at[row])] + moved[row]
        for row in rows:
            upper = along_z([sums[row, half, 0] + sums[row, half, 1] for half in (0, 1)], 1)
            for half in (0, 1):
                at = tile((row, half))
                force = (sums[row, half, 0] - sums[row, half, 1]) + upper[half]
                value = step_ref[(plane, *at)] * force + shift_ref[(plane, *at)] * w_ref[(c, plane, *at)]
                if older_ref is None:
                    value = 0.5 * value
                else:
                    value = value - older_ref[(c, plane, *at)]
                out_ref[(c, plane, *at)] = value


def coefficients(nu):
    half = 0.5

    def gram(i, j):
        return half * (nu[i + j] + nu[abs(i - j)])

    def image(p):
        out = [None] * (len(p) + 1)

        def add(i, value):
            out[i] = value if out[i] is None else out[i] + value

        for k, value in enumerate(p):
            whole, part = SIGMA * value, (0.5 * SIGMA) * value
            add(k, whole)
            if k == 0:
                add(1, whole)
            else:
                add(k + 1, part)
                add(k - 1, part)
        return out

    def form(u, v):
        total = None
        for i, ui in enumerate(u):
            row = None
            for j, vj in enumerate(v):
                term = gram(i, j) * vj
                row = term if row is None else row + term
            total = ui * row if total is None else total + ui * row
        return total

    one = jnp.ones_like(nu[0])
    solution, residual, direction = [], [one], [one]
    descent = gram(0, 0)
    for iteration in range(ITERS):
        moved = image(direction)
        step = descent / form(direction, moved)
        solution = [
            step * p + (solution[k] if k < len(solution) else 0.0) for k, p in enumerate(direction)
        ]
        residual = [
            (residual[k] - step * m) if k < len(residual) else -(step * m)
            for k, m in enumerate(moved)
        ]
        if iteration + 1 < ITERS:
            new = form(residual, residual)
            ratio = new / descent
            direction = [
                r + ratio * direction[k] if k < len(direction) else r
                for k, r in enumerate(residual)
            ]
            descent = new
    return solution, residual


def place(x, y, z, core):
    return {"gx": ((y // 2) * 4 + x) * 2 + core, "gy": lax.rem(y, 2) * 8 + z}


def kernel(r_hbm, l_hbm, w0, w1, w2, w3, w4, diag, factors, r_in, labels, step_ref, shift_ref, below,
           *rest):
    sets, rest = [rest[5 * k : 5 * k + 5] for k in range(3)], rest[15:]
    (from_x, from_y, from_xy, mine, theirs, load_sem, send_sem, recv_sem,
     face_send, face_recv, edge_send, edge_recv, sum_send, sum_recv) = rest
    gx, gy = lax.axis_index("gx"), lax.axis_index("gy")
    core, x, y_hi = lax.rem(gx, 2), lax.rem(gx // 2, 4), gx // 8
    z, y_lo = lax.rem(gy, 8), gy // 8
    y = y_hi * 2 + y_lo

    def neighbour(dx, dy):
        return {"gx": lax.rem(gx + dx + GROUP, GROUP), "gy": lax.rem(gy + dy + GROUP, GROUP)}

    stages = [
        [place(x, y, lax.rem(z + k // 2, 8), lax.rem(core + k % 2, 2)) for k in range(1, GROUP)],
        [place(lax.rem(x + k // 4, 4), lax.rem(y + k % 4, 4), z, core) for k in range(1, GROUP)],
    ]
    barrier = pltpu.get_barrier_semaphore()
    greeted = [neighbour(dx, dy) for dx, dy in DIRECTIONS] + stages[0] + stages[1]
    for device in greeted:
        pl.semaphore_signal(barrier, inc=1, device_id=device, device_id_type=MESH)
    own = (pl.ds(HALO, NX), pl.ds(0, NY))
    load_r = pltpu.make_async_copy(r_hbm, r_in.at[:, own[0], own[1]], load_sem.at[0])
    load_l = pltpu.make_async_copy(l_hbm, labels.at[own[0], own[1]], load_sem.at[1])
    load_r.start()
    load_l.start()
    load_r.wait()
    load_l.wait()
    pl.semaphore_wait(barrier, len(greeted))

    def piece(xs, ys, xd, yd, device, sends, recvs):
        pairs = ((labels.at[xs, ys], labels.at[xd, yd]), (r_in.at[:, xs, ys], r_in.at[:, xd, yd]))
        return [
            pltpu.make_async_remote_copy(
                src_ref=source, dst_ref=target, send_sem=sends(kind), recv_sem=recvs(kind),
                device_id=device, device_id_type=MESH,
            )
            for kind, (source, target) in enumerate(pairs)
        ]

    def rows(dy):
        return (pl.ds({1: 4, 0: 0, -1: 0}[dy], NY if dy == 0 else 4),
                pl.ds({1: 12, 0: 0, -1: 8}[dy], NY if dy == 0 else 4))

    def slab(number):
        dx, dy = DIRECTIONS[number]
        ys, yd = rows(dy)
        return piece(
            pl.ds(NX if dx == 1 else HALO, HALO), ys, pl.ds(0 if dx == 1 else HALO + NX, HALO), yd,
            neighbour(dx, dy),
            lambda kind: send_sem.at[kind, number], lambda kind: recv_sem.at[kind, number],
        )

    def face(part, side):
        ys, yd = rows(1 - 2 * side)
        at = pl.ds(2 * part + 2, 2)
        return piece(
            at, ys, at, yd, neighbour(0, 1 - 2 * side),
            lambda kind: face_send.at[kind, side, part - 1],
            lambda kind: face_recv.at[kind, side, part - 1],
        )

    halo = []
    for number in (0, 1, 2):
        halo += slab(number)
    for part in range(1, 9):
        halo += face(part, 0) + face(part, 1)
    for number in (3, 4, 5):
        halo += slab(number)
    for copy in halo:
        copy.start()

    def corner_sums(plane):
        value = pick(labels[plane] > 0, lambda la, mu: (la + 4.0 * mu) / 9.0)
        value = value + pltpu.roll(value, 1, 1)
        return value + pltpu.roll(value, 1, 0)

    def diagonal_plane(plane):
        here = corner_sums(plane)
        value = here + below[...] + KAPPA
        below[...] = here
        inverse = 1.0 / value
        diag[plane] = value
        step = STEP * inverse
        step_ref[plane] = step
        shift_ref[plane] = (RAW * KAPPA) * step - 2.0
        for c in range(3):
            w0[c, plane] = r_in[c, plane] * inverse

    basis = (w0, w1, w2, w3, w4)

    def modes_of(k, plane, parity, tiles=TILES, ref=None):
        ref = basis[k - 1] if ref is None else ref
        plane_modes(ref, plane, sets[k - 1][parity], tiles)

    def forces_of(k, plane, parity):
        group = sets[k - 1]
        voxel_forces(plane, labels, group[parity], group[1 - parity], group[4],
                     group[2 + parity])

    def next_of(k, plane, parity):
        group, older = sets[k - 1], basis[k - 2] if k > 1 else None
        next_basis(plane, group[2 + parity], step_ref, shift_ref,
                   basis[k - 1], older, basis[k])

    def level(k, plane, parity, count):
        for i in range(count):
            modes_of(k, plane + i + 1, (parity + i + 1) % 2)
            forces_of(k, plane + i, (parity + i) % 2)
        for i in range(count):
            next_of(k, plane + i, (parity + i) % 2)

    def arrived(copies):
        for copy in copies:
            copy.wait_recv()

    def levels(first, which):
        for k in which:
            level(k, first - 3 * k, k % 2, 2)

    def diagonals(first):
        for extra in (0, 1):
            diagonal_plane(first + extra)

    below[...] = jnp.zeros_like(below)
    arrived(slab(0) + slab(1) + slab(2))
    diagonals(0)
    diagonals(2)
    modes_of(1, 1, 1)
    levels(4, (1,))
    arrived(face(1, 0) + face(1, 1))
    diagonals(4)
    modes_of(2, 2, 0)
    levels(6, (1,))
    arrived(face(2, 0) + face(2, 1))
    diagonals(6)
    levels(8, (2, 1))
    arrived(face(3, 0) + face(3, 1))
    diagonals(8)
    modes_of(3, 3, 1)
    levels(10, (2, 1))
    arrived(face(4, 0) + face(4, 1))
    diagonals(10)

    def steady(number, _):
        first = 12 + 2 * number

        @pl.when(first < HALO + NX)
        def _():
            part = first // 2 - 1
            arrived(face(part, 0) + face(part, 1))

        @pl.when(first == HALO + NX)
        def _():
            arrived(slab(3) + slab(4) + slab(5))

        levels(first, (3, 2, 1))
        diagonals(first)
        return 0

    lax.fori_loop(0, 6, steady, 0)
    levels(24, (3, 2, 1))
    levels(26, (3, 2))
    levels(28, (3,))

    edges = [
        (w3.at[:, pl.ds(HALO + NX - 1, 1)], from_x, (1, 0)),
        (w3.at[:, pl.ds(HALO, NX + 1), pl.ds(NY - 1, 1)], from_y.at[:, :, pl.ds(NY - 1, 1)], (0, 1)),
        (w3.at[:, pl.ds(HALO + NX - 1, 1), pl.ds(0, NY)], from_xy, (1, 1)),
    ]
    edge_copies = []
    for number, (source, target, (dx, dy)) in enumerate(edges):
        copy = pltpu.make_async_remote_copy(
            src_ref=source, dst_ref=target,
            send_sem=edge_send.at[number], recv_sem=edge_recv.at[number],
            device_id=neighbour(dx, dy), device_id_type=MESH,
        )
        copy.start()
        edge_copies.append(copy)

    zero = jnp.zeros((NY, 128), jnp.float32)
    near = TILES[:2]
    modes_of(1, HALO, 0, near, w3)

    def inner(plane, parity, sums):
        sums = list(sums)
        modes_of(1, plane + 1, 1 - parity, near, w3)
        lower, upper = sets[0][parity], sets[0][1 - parity]
        for lane in (0, 128):
            at = (slice(0, NY), slice(lane, lane + 128))
            weight = diag[plane, at[0], at[1]]
            for c in range(3):
                w = [ref[c, plane, at[0], at[1]] for ref in basis[:4]]
                scaled = [weight * v for v in w]
                for i, (j, k) in enumerate(DOTS):
                    sums[i] = sums[i] + scaled[j] * w[k]
                sums[7] = sums[7] + (RAW * KAPPA) * (w[3] * w[3])
            sums[7] = sums[7] + voxel_energy(plane, labels, at, lower, upper)
        return tuple(sums)

    def inner_two(number, sums):
        plane = HALO + 2 * number
        sums = inner(plane, 0, sums)
        return inner(plane + 1, 1, sums)

    sums = lax.fori_loop(0, NX // 2, inner_two, (zero,) * 8)
    lane = lax.broadcasted_iota(jnp.int32, (1, 128), 1)
    row = jnp.zeros((1, 128), jnp.float32)
    for i, value in enumerate(sums):
        value = jnp.sum(jnp.sum(value, axis=0, keepdims=True), axis=1, keepdims=True)
        row = jnp.where(lane == i, value, row)

    def share(stage, row):
        mine[stage] = row
        copies = []
        for number, device in enumerate(stages[stage]):
            copy = pltpu.make_async_remote_copy(
                src_ref=mine.at[stage], dst_ref=theirs.at[stage, number],
                send_sem=sum_send.at[stage, number], recv_sem=sum_recv.at[stage, number],
                device_id=device, device_id_type=MESH,
            )
            copy.start()
            copies.append(copy)
        return copies

    def collect(stage, row, copies):
        for copy in copies:
            copy.wait()
        for number in range(len(copies)):
            row = row + theirs[stage, number]
        return row

    copies = share(0, row)
    for copy in halo:
        copy.wait_send()
    for copy in edge_copies:
        copy.wait()
    for c in range(3):
        w3[c, HALO - 1, 0:8] = from_x[c, 0, 0:8]
        w3[c, HALO - 1, 8:16] = from_x[c, 0, 8:16]
        w3[c, HALO - 1, 15:16] = from_xy[c, 0, 7:8]
        for plane in range(NX + 1):
            w3[c, HALO + plane, 15:16] = from_y[c, plane, 7:8]
    row = collect(0, row, copies)
    copies = share(1, row)

    def last_level(plane, parity):
        modes_of(1, plane + 1, 1 - parity, TILES, w3)
        forces_of(1, plane, parity)
        next_basis(plane, sets[0][2 + parity], step_ref, shift_ref,
                   w3, w2, w4, (0,))

    def last_two(number, _):
        plane = HALO - 1 + 2 * number
        last_level(plane, 1)
        last_level(plane + 1, 0)
        return 0

    modes_of(1, HALO - 1, 1, TILES, w3)
    lax.fori_loop(0, NX // 2, last_two, 0)
    last_level(HALO + NX - 1, 1)

    row = collect(1, row, copies)
    dots = [
        jnp.sum(jnp.where(lane == i, row, 0.0), axis=1, keepdims=True) for i in range(8)
    ]
    last = (2.0 / (RAW * SIGMA)) * dots[7] - 2.0 * dots[6] - dots[5]
    nu = [
        dots[0], dots[1], 2.0 * dots[2] - dots[0], 2.0 * dots[3] - dots[1],
        2.0 * dots[4] - dots[0], 2.0 * dots[5] - dots[1], 2.0 * dots[6] - dots[0],
        2.0 * last - dots[1],
    ]
    solution, residual = coefficients(nu)
    for k, value in enumerate(solution + residual):
        factors[k] = jnp.broadcast_to(value, (NY, 128))


PART = 4


def combine(w0, w1, w2, w3, w4, diag, factors, sol_hbm, res_hbm, sol, res, sems):
    basis = (w0, w1, w2, w3, w4)
    solution = [factors[k] for k in range(4)]
    residual = [factors[4 + k] for k in range(5)]
    copies = []
    for part in range(NX // PART):
        def one(number, _):
            plane = HALO + number
            for c in range(3):
                for lane in (0, 128):
                    at = (slice(0, NY), slice(lane, lane + 128))
                    w = [ref[c, plane, at[0], at[1]] for ref in basis]
                    x = solution[0] * w[0]
                    r = residual[0] * w[0]
                    for k in range(1, 5):
                        if k < 4:
                            x = x + solution[k] * w[k]
                        r = r + residual[k] * w[k]
                    sol[c, number, at[0], at[1]] = x
                    res[c, number, at[0], at[1]] = diag[plane, at[0], at[1]] * r
            return 0

        lax.fori_loop(part * PART, part * PART + PART, one, 0)
        planes = pl.ds(part * PART, PART)
        for i, (source, target) in enumerate(((sol, sol_hbm), (res, res_hbm))):
            copy = pltpu.make_async_copy(source.at[:, planes], target.at[:, planes], sems.at[i, part])
            copy.start()
            copies.append(copy)
    for copy in copies:
        copy.wait()


def local(right_side, labels):
    shape = (3, NX, NY, NZ)
    wide = jax.ShapeDtypeStruct((3, PX, PY, NZ), jnp.float32)
    vector = pltpu.VMEM((3, PX, PY, NZ), jnp.float32)
    in_vmem = pl.BlockSpec(memory_space=pltpu.VMEM)
    in_hbm = pl.BlockSpec(memory_space=pltpu.HBM)
    scalar = pltpu.VMEM((PX, PY, NZ), jnp.float32)
    modes = pltpu.VMEM((12, PY, NZ), jnp.float32)
    parts = pl.pallas_call(
        kernel,
        out_shape=(*([wide] * 5), jax.ShapeDtypeStruct((PX, PY, NZ), jnp.float32),
                   jax.ShapeDtypeStruct((9, NY, 128), jnp.float32)),
        in_specs=[in_hbm] * 2,
        out_specs=[in_vmem] * 7,
        scratch_shapes=[
            vector, pltpu.VMEM((PX, PY, NZ), jnp.int32), scalar, scalar,
            pltpu.VMEM((PY, NZ), jnp.float32),
            *([modes] * 15),
            pltpu.VMEM((3, 1, PY, NZ), jnp.float32),
            pltpu.VMEM((3, NX + 1, NY, NZ), jnp.float32),
            pltpu.VMEM((3, 1, NY, NZ), jnp.float32),
            pltpu.VMEM((2, 1, 128), jnp.float32),
            pltpu.VMEM((2, GROUP - 1, 1, 128), jnp.float32),
            pltpu.SemaphoreType.DMA((2,)),
            pltpu.SemaphoreType.DMA((2, 6)),
            pltpu.SemaphoreType.DMA((2, 6)),
            pltpu.SemaphoreType.DMA((2, 2, 8)),
            pltpu.SemaphoreType.DMA((2, 2, 8)),
            pltpu.SemaphoreType.DMA((3,)),
            pltpu.SemaphoreType.DMA((3,)),
            pltpu.SemaphoreType.DMA((2, GROUP - 1)),
            pltpu.SemaphoreType.DMA((2, GROUP - 1)),
        ],
        compiler_params=pltpu.CompilerParams(
            collective_id=0, has_side_effects=True, vmem_limit_bytes=24 * 1024 * 1024
        ),
    )(*(pltpu.with_memory_space_constraint(a, pltpu.HBM) for a in (right_side, labels)))
    block = pltpu.VMEM(shape, jnp.float32)
    return pl.pallas_call(
        combine,
        out_shape=(jax.ShapeDtypeStruct(shape, jnp.float32),) * 2,
        in_specs=[in_vmem] * 7,
        out_specs=[in_hbm] * 2,
        scratch_shapes=[block, block, pltpu.SemaphoreType.DMA((2, NX // PART))],
        compiler_params=pltpu.CompilerParams(vmem_limit_bytes=8 * 1024 * 1024),
    )(*parts)


def solution(mesh):
    specs = P(None, "gx", "gy", None)
    return jax.shard_map(
        local, mesh=mesh, in_specs=(specs, P("gx", "gy", None)), out_specs=(specs, specs),
        check_vma=False,
    )
```
